128 devices in a mesh: rep: 1, sub: 16 (over z, y), blk: 8 (over x, core).
Axes of the slice: x: 4, y: 4, z: 4, core: 2. Of those that a mesh axis runs over, the one named last changes fastest.
Arguments:
- ratings: float32 [262144, 512], P(('rep', 'blk', 'sub'))
- mask: int32 [262144, 512], P(('rep', 'blk', 'sub'))
- user_init: float32 [262144, 32], P(('rep', 'blk', 'sub'))
- item_init: float32 [512, 32], P(('rep', 'blk'))
Outputs:
- output 1: float32 [262144, 32], P(('rep', 'blk', 'sub'))
- output 2: float32 [512, 32], P(('rep', 'blk'))
All inputs are finite; a program needn't handle non-finite values.
Results may differ from the reference program's by a relative error of at most 0.001.
Values are sent between devices in bfloat16 or wider.
A program may use at most 1 GiB of HBM per device.

```python
import math
import jax
import jax.numpy as jnp
from jax import lax

BLOCKS = 8
SUB_SHARDS = 16
USERS_DEV = 2048
ITEMS_DEV = 64
RANK = 32
STEPS = 4
EPOCHS = 2

USERS_BLK = SUB_SHARDS * USERS_DEV
USERS = BLOCKS * USERS_BLK
ITEMS = BLOCKS * ITEMS_DEV
BIG_SIDE = max(ITEMS_DEV, USERS_BLK)
STEP_SIZE = 0.4 * math.sqrt(RANK) / (math.sqrt(BIG_SIDE) + math.sqrt(RANK)) ** 2
WEIGHT_DECAY = 0.002 / STEP_SIZE


def setup_inputs(seed: int = 0, part: int = 0) -> dict:
    part_key = jax.random.fold_in(jax.random.key(seed), part)
    keys = jax.random.split(part_key, 7)
    user_true = jax.random.normal(keys[0], (USERS, RANK), jnp.float32)
    item_true = jax.random.normal(keys[1], (ITEMS, RANK), jnp.float32)
    noise = jax.random.normal(keys[2], (USERS, ITEMS), jnp.float32)
    ratings = jnp.dot(user_true, item_true.T) / math.sqrt(RANK) + 0.3 * noise
    block_pct = jax.random.randint(keys[3], (BLOCKS, 1, BLOCKS, 1), 10, 51)
    draws = jax.random.randint(keys[4], (BLOCKS, USERS_BLK, BLOCKS, ITEMS_DEV), 0, 100)
    mask = (draws < block_pct).astype(jnp.int32).reshape(USERS, ITEMS)
    init_scale = RANK ** -0.25
    user_init = jax.random.normal(keys[5], (USERS, RANK), jnp.float32) * init_scale
    item_init = jax.random.normal(keys[6], (ITEMS, RANK), jnp.float32) * init_scale
    return {'ratings': ratings, 'mask': mask, 'user_init': user_init, 'item_init': item_init}


def reference(ratings, mask, user_init, item_init):
    rating_blk = ratings.reshape(BLOCKS, USERS_BLK, BLOCKS, ITEMS_DEV)
    mask_blk = mask.reshape(BLOCKS, USERS_BLK, BLOCKS, ITEMS_DEV).astype(jnp.float32)
    block_ids = jnp.arange(BLOCKS)

    def sub_epoch(state, offset):
        cols = (block_ids + offset) % BLOCKS
        rating_now = rating_blk[block_ids, :, cols, :]
        mask_now = mask_blk[block_ids, :, cols, :]

        def grad_step(inner, unused):
            users, items = inner
            user_half = users.astype(jnp.bfloat16).astype(jnp.float32)
            item_half = items.astype(jnp.bfloat16).astype(jnp.float32)
            predicted = jnp.einsum('bur,bir->bui', user_half, item_half)
            err_half = (mask_now * (predicted - rating_now)).astype(jnp.bfloat16).astype(jnp.float32)
            grad_user = jnp.einsum('bui,bir->bur', err_half, item_half) + WEIGHT_DECAY * users
            grad_item = jnp.einsum('bui,bur->bir', err_half, user_half) + WEIGHT_DECAY * items
            return (users - STEP_SIZE * grad_user, items - STEP_SIZE * grad_item), None

        inner, unused = lax.scan(grad_step, state, None, length=STEPS)
        return (inner[0], jnp.roll(inner[1], -1, axis=0)), None

    start = (user_init.reshape(BLOCKS, USERS_BLK, RANK), item_init.reshape(BLOCKS, ITEMS_DEV, RANK))
    offsets = jnp.tile(block_ids, EPOCHS)
    final, unused = lax.scan(sub_epoch, start, offsets)
    return final[0].reshape(USERS, RANK), final[1].reshape(ITEMS, RANK)
```

```python
import functools
import math

import jax
import jax.numpy as jnp
from jax import lax
from jax.experimental import pallas as pl
from jax.experimental.pallas import tpu as pltpu
from jax.sharding import PartitionSpec as P

STEPS = 4
EPOCHS = 2
STEP_GAIN = 0.4
DECAY = 0.002
GROUPS = 4
MESH = pl.DeviceIdType.MESH
OFFSETS = ((2, 2), (2, 1), (2, 3), (1, 2), (3, 2), (1, 1), (1, 3), (3, 1), (3, 3), (2, 0), (0, 2), (1, 0), (3, 0), (0, 1), (0, 3))


def kernel(dims, r_hbm, m_hbm, ut_in, vt_in, ut_out, vt_out, rbuf, mbuf, packed, ut, uh, uth, wt, err, vst, xsend, slots, xslots, vslots,
           load_sem, send_sem, recv_sem, xsend_sem, xrecv_sem, vsend_sem, vrecv_sem):
    blk_n, sub_n, step_size, decay_coef = dims
    users = ut_in.shape[1]
    rows = users // GROUPS
    rank = ut_in.shape[0]
    half = rank // 2
    pairs = blk_n // 2
    me_b = lax.axis_index("blk")
    me_s = lax.axis_index("sub")
    me_z, me_y = me_s // 4, me_s % 4
    prev_b = (me_b + blk_n - 1) % blk_n
    next_b = (me_b + 1) % blk_n
    first_pair = me_b // 2

    def load(q, src, dst, sem):
        col = pl.multiple_of(((first_pair + q) % pairs) * 128, 128)
        return pltpu.make_async_copy(src.at[:, pl.ds(col, 128)], dst.at[q], load_sem.at[sem, q])

    for q in range(pairs):
        load(q, r_hbm, rbuf, 0).start()
        load(q, m_hbm, mbuf, 1).start()

    def at(dz, dy):
        return ((me_z + dz) % 4) * 4 + (me_y + dy) % 4

    barrier = pltpu.get_barrier_semaphore()
    for dz, dy in OFFSETS:
        pl.semaphore_signal(barrier, inc=1, device_id={"sub": at(dz, dy)}, device_id_type=MESH)
    for other in (prev_b, next_b):
        for dz, dy in OFFSETS + ((0, 0),):
            pl.semaphore_signal(barrier, inc=1, device_id={"sub": at(dz, dy), "blk": other}, device_id_type=MESH)

    low = lax.broadcasted_iota(jnp.int32, (half, 128), 1) < 64

    for g in range(GROUPS):
        piece = ut_in[:, g * rows:(g + 1) * rows]
        ut[g * rank:(g + 1) * rank, :] = piece
    first = ut[...].astype(jnp.bfloat16)
    uth[...] = first
    uh[...] = first.T
    vst[:, 0:64] = vt_in[0:half, :]
    vst[:, 64:128] = vt_in[half:rank, :]
    wt[...] = jnp.zeros_like(wt)

    chunk = 64
    low_c = lax.broadcasted_iota(jnp.int32, (chunk, 128), 1) < 64

    def pack_pair(q, carry):
        load(q, r_hbm, rbuf, 0).wait()
        load(q, m_hbm, mbuf, 1).wait()
        even = ((first_pair + q) % pairs) * 2

        def pack_rows(c, carry2):
            base = pl.multiple_of(c * chunk, chunk)
            for col in range(2):
                vals = []
                for g in (2 * col, 2 * col + 1):
                    src = pl.ds(g * rows + base, chunk)
                    vals.append(jnp.where(mbuf[q, src, :] != 0, rbuf[q, src, :], jnp.nan))
                x0, x1 = vals
                packed[even, pl.ds(base, chunk), col * 128:(col + 1) * 128] = jnp.where(low_c, x0, pltpu.roll(x1, 64, 1))
                packed[even + 1, pl.ds(base, chunk), col * 128:(col + 1) * 128] = jnp.where(low_c, pltpu.roll(x0, 64, 1), x1)
            return carry2

        lax.fori_loop(0, rows // chunk, pack_rows, 0)
        return carry

    lax.fori_loop(0, pairs, pack_pair, 0)
    pl.semaphore_wait(barrier, 3 * sub_n - 1)

    def spread(vp):
        swapped = pltpu.roll(vp, 64, 1)
        full = jnp.concatenate([jnp.where(low, vp, swapped), jnp.where(low, swapped, vp)], axis=0)
        left = lax.broadcasted_iota(jnp.int32, (rank, 128), 1) < 64
        lo = jnp.where(left, full, 0.0).astype(jnp.bfloat16)
        hi = jnp.where(left, 0.0, full).astype(jnp.bfloat16)
        wt[0:rank, 0:128] = lo
        wt[rank:2 * rank, 0:128] = hi
        wt[2 * rank:3 * rank, 128:256] = lo
        wt[3 * rank:4 * rank, 128:256] = hi

    def partial(block):
        for c in range(2):
            sl = slice(c * (rows // 2), (c + 1) * (rows // 2))
            predicted = jnp.dot(uh[sl, :], wt[...], preferred_element_type=jnp.float32)
            rate = packed[block, sl, :]
            err[sl, :] = jnp.where(rate == rate, predicted - rate, 0.0).astype(jnp.bfloat16)
        z = jnp.dot(uth[...], err[...], preferred_element_type=jnp.float32)
        s_lo = z[0:rank, 0:128] + z[2 * rank:3 * rank, 128:256]
        s_hi = z[rank:2 * rank, 0:128] + z[3 * rank:4 * rank, 128:256]
        left = lax.broadcasted_iota(jnp.int32, (rank, 128), 1) < 64
        both = jnp.where(left, s_lo, s_hi)
        top, bottom = both[0:half], both[half:rank]
        return jnp.where(low, top, bottom) + pltpu.roll(jnp.where(low, bottom, top), 64, 1)

    def user_step():
        grad = lax.dot_general(wt[...], err[...], (((1,), (1,)), ((), ())), preferred_element_type=jnp.float32)
        old = ut[...]
        new = old - step_size * (grad + decay_coef * old)
        ut[...] = new
        new_half = new.astype(jnp.bfloat16)
        uth[...] = new_half
        uh[...] = new_half.T

    def item_step(parts):
        total = parts[0]
        for s in range(1, sub_n):
            total = total + parts[s]
        old = vst[...]
        return old - step_size * (total + decay_coef * old)

    def sub_epoch(t, carry):
        block = (me_b + t) % blk_n
        for step in range(STEPS - 1):
            spread(vst[...])
            slots[step, me_s] = partial(block)
            copies = []
            for dz, dy in OFFSETS:
                copy = pltpu.make_async_remote_copy(
                    src_ref=slots.at[step, me_s], dst_ref=slots.at[step, me_s], send_sem=send_sem.at[step], recv_sem=recv_sem.at[step],
                    device_id={"sub": at(dz, dy)}, device_id_type=MESH)
                copy.start()
                copies.append(copy)
            user_step()
            everyone = slots.at[step, pl.ds(0, sub_n - 1)]
            pltpu.make_async_copy(everyone, everyone, send_sem.at[step]).wait()
            pltpu.make_async_copy(everyone, everyone, recv_sem.at[step]).wait()
            vst[...] = item_step(slots[step])
        ahead = pltpu.make_async_remote_copy(
            src_ref=vst, dst_ref=vslots.at[t], send_sem=vsend_sem, recv_sem=vrecv_sem.at[t],
            device_id={"blk": prev_b}, device_id_type=MESH)
        ahead.start()
        spread(vst[...])
        xsend[...] = partial(block)
        for dz, dy in OFFSETS + ((0, 0),):
            pltpu.make_async_remote_copy(
                src_ref=xsend, dst_ref=xslots.at[t, me_s], send_sem=xsend_sem, recv_sem=xrecv_sem.at[t],
                device_id={"sub": at(dz, dy), "blk": prev_b}, device_id_type=MESH).start()
        user_step()
        everyone = xslots.at[t]
        pltpu.make_async_copy(everyone, everyone, xsend_sem).wait()
        ahead.wait()
        pltpu.make_async_copy(everyone, everyone, xrecv_sem.at[t]).wait()
        vst[...] = vslots[t]
        vst[...] = item_step(xslots[t])
        return carry

    lax.fori_loop(0, EPOCHS * blk_n, sub_epoch, 0)

    for g in range(GROUPS):
        ut_out[:, g * rows:(g + 1) * rows] = ut[g * rank:(g + 1) * rank, :]
    vt_out[0:half, :] = vst[:, 0:64]
    vt_out[half:rank, :] = vst[:, 64:128]


def solution(mesh):
    blk_n = mesh.shape["blk"]
    sub_n = mesh.shape["sub"]
    row_spec = P(("rep", "blk", "sub"), None)
    item_spec = P(("rep", "blk"), None)

    def local_run(ratings, mask, user_init, item_init):
        users = ratings.shape[0]
        items, rank = item_init.shape
        big_side = max(items, sub_n * users)
        step_size = STEP_GAIN * math.sqrt(rank) / (math.sqrt(big_side) + math.sqrt(rank)) ** 2
        decay_coef = DECAY / step_size
        rows = users // GROUPS
        turns = EPOCHS * blk_n
        half = rank // 2
        vmem = pl.BlockSpec(memory_space=pltpu.VMEM)
        ut, vt = pl.pallas_call(
            functools.partial(kernel, (blk_n, sub_n, step_size, decay_coef)),
            out_shape=(jax.ShapeDtypeStruct((rank, users), jnp.float32), jax.ShapeDtypeStruct((rank, items), jnp.float32)),
            in_specs=[pl.BlockSpec(memory_space=pl.ANY)] * 2 + [vmem] * 2,
            out_specs=(vmem, vmem),
            scratch_shapes=[
                pltpu.VMEM((blk_n // 2, users, 128), jnp.float32),
                pltpu.VMEM((blk_n // 2, users, 128), jnp.int32),
                pltpu.VMEM((blk_n, rows, GROUPS * items), jnp.float32),
                pltpu.VMEM((GROUPS * rank, rows), jnp.float32),
                pltpu.VMEM((rows, GROUPS * rank), jnp.bfloat16),
                pltpu.VMEM((GROUPS * rank, rows), jnp.bfloat16),
                pltpu.VMEM((GROUPS * rank, GROUPS * items), jnp.bfloat16),
                pltpu.VMEM((rows, GROUPS * items), jnp.bfloat16),
                pltpu.VMEM((half, 128), jnp.float32),
                pltpu.VMEM((half, 128), jnp.float32),
                pltpu.VMEM((STEPS - 1, sub_n, half, 128), jnp.float32),
                pltpu.VMEM((turns, sub_n, half, 128), jnp.float32),
                pltpu.VMEM((turns, half, 128), jnp.float32),
                pltpu.SemaphoreType.DMA((2, blk_n // 2)),
                pltpu.SemaphoreType.DMA((STEPS - 1,)),
                pltpu.SemaphoreType.DMA((STEPS - 1,)),
                pltpu.SemaphoreType.DMA,
                pltpu.SemaphoreType.DMA((turns,)),
                pltpu.SemaphoreType.DMA,
                pltpu.SemaphoreType.DMA((turns,)),
            ],
            compiler_params=pltpu.CompilerParams(collective_id=0, has_side_effects=True, vmem_limit_bytes=48 * 1024 * 1024),
        )(ratings, mask, user_init.T, item_init.T)
        return ut.T, vt.T

    return jax.shard_map(local_run, mesh=mesh, in_specs=(row_spec, row_spec, row_spec, item_spec), out_specs=(row_spec, item_spec), check_vma=False)
```

```python
import functools
import math

import jax
import jax.numpy as jnp
from jax import lax
from jax.experimental import pallas as pl
from jax.experimental.pallas import tpu as pltpu
from jax.sharding import PartitionSpec as P

STEPS = 4
EPOCHS = 2
STEP_GAIN = 0.4
DECAY = 0.002
GROUPS = 4
TEAM = 4
PIECES = 4
MESH = pl.DeviceIdType.MESH


def kernel(dims, r_hbm, m_hbm, u_hbm, v_hbm, ut_out, vt_out, rbuf, mbuf, ubuf, vbuf, packed, work, usrc, uret, vown, vret, ut, uh, uth, wt, err, vst,
           xsend, slots, xslots, vslots, load_sem, ship_send, ship_recv, user_send, user_recv, item_send, item_recv, back_send, back_recv,
           final_send, final_recv, send_sem, recv_sem, xsend_sem, xrecv_sem, vsend_sem, vrecv_sem):
    blk_n, step_size, decay_coef = dims
    rank, users = ubuf.shape
    rows = users // GROUPS
    half = rank // 2
    pairs = blk_n // 2
    me_b = lax.axis_index("blk")
    me_s = lax.axis_index("sub")
    x, core = me_b // 2, me_b % 2
    z, y = me_s // 4, me_s % 4

    out_y = (y // 2 + core + x) % 2
    out_z = z // 2
    piece = 2 * out_y + out_z
    target = {"sub": (z + out_z * (3 - 2 * z)) * 4 + y + out_y * (3 - 2 * y), "blk": 2 * x + 1}
    is_own = jnp.logical_and(core == 1, piece == 0)
    ships = jnp.logical_not(is_own)
    is_worker = jnp.logical_and(core == 1, z < 2)
    job_core = (y // 2 + x) % 2
    job = 2 * x + job_core
    has_own = job_core == 1
    place = (z % 2) * 2 + y % 2

    def source(q):
        oy, oz = q // 2, q % 2
        return {"sub": (z + oz * (3 - 2 * z)) * 4 + y + oy * (3 - 2 * y), "blk": job}

    def worker(block, p):
        bx = block // 2
        return {"sub": (p // 2) * 4 + 2 * ((block % 2 + bx) % 2) + p % 2, "blk": 2 * bx + 1}

    prev_job = (job + blk_n - 1) % blk_n
    next_job = (job + 1) % blk_n

    def mate(d):
        dz, dy = d // 2, d % 2
        pz, py = (place // 2 + dz) % 2, (place % 2 + dy) % 2
        return pz * 2 + py

    def load(q, src, dst, kind):
        col = pl.multiple_of(((x + q) % pairs) * 128, 128)
        return pltpu.make_async_copy(src.at[:, pl.ds(col, 128)], dst.at[q], load_sem.at[kind, q])

    load_users = pltpu.make_async_copy(u_hbm, ubuf, load_sem.at[2, 0])
    load_items = pltpu.make_async_copy(v_hbm, vbuf, load_sem.at[2, 1])
    load_users.start()
    load_items.start()
    for q in range(pairs):
        load(q, r_hbm, rbuf, 0).start()
        load(q, m_hbm, mbuf, 1).start()

    barrier = pltpu.get_barrier_semaphore()

    def greet(device):
        pl.semaphore_signal(barrier, inc=1, device_id=device, device_id_type=MESH)

    @pl.when(ships)
    def _():
        greet(target)

    @pl.when(is_worker)
    def _():
        for q in range(1, PIECES):
            greet(source(q))

        @pl.when(jnp.logical_not(has_own))
        def _():
            greet(source(0))

        for d in (3, 2, 1):
            greet(worker(job, mate(d)))
        for p in range(TEAM):
            greet(worker(prev_job, p))
            greet(worker(next_job, p))

    low = lax.broadcasted_iota(jnp.int32, (half, 128), 1) < 64
    left = lax.broadcasted_iota(jnp.int32, (rank, 128), 1) < 64

    load_users.wait()
    for g in range(GROUPS):
        usrc[g * rank:(g + 1) * rank, :] = ubuf[:, g * rows:(g + 1) * rows]
    load_items.wait()
    vown[:, 0:64] = vbuf[0:half, :]
    vown[:, 64:128] = vbuf[half:rank, :]

    @pl.when(jnp.logical_not(is_worker))
    def _():
        pl.semaphore_wait(barrier, 1)

    @pl.when(jnp.logical_and(is_worker, has_own))
    def _():
        pl.semaphore_wait(barrier, PIECES - 1 + TEAM - 1 + 2 * TEAM)

    @pl.when(jnp.logical_and(is_worker, jnp.logical_not(has_own)))
    def _():
        pl.semaphore_wait(barrier, PIECES + 1 + TEAM - 1 + 2 * TEAM)

    send_users = pltpu.make_async_remote_copy(
        src_ref=usrc, dst_ref=ut.at[piece], send_sem=user_send, recv_sem=user_recv, device_id=target, device_id_type=MESH)
    send_items = pltpu.make_async_remote_copy(
        src_ref=vown, dst_ref=vst, send_sem=item_send, recv_sem=item_recv, device_id=target, device_id_type=MESH)
    gives_items = jnp.logical_and(core == 0, piece == 0)

    @pl.when(ships)
    def _():
        send_users.start()

    @pl.when(gives_items)
    def _():
        send_items.start()

    def ship(k):
        column = (me_b + k) % blk_n
        return pltpu.make_async_remote_copy(
            src_ref=packed.at[column], dst_ref=work.at[column, piece], send_sem=ship_send.at[k], recv_sem=ship_recv.at[column],
            device_id=target, device_id_type=MESH)

    chunk = 64
    low_c = lax.broadcasted_iota(jnp.int32, (chunk, 128), 1) < 64

    def pack_pair(q):
        load(q, r_hbm, rbuf, 0).wait()
        load(q, m_hbm, mbuf, 1).wait()
        even = ((x + q) % pairs) * 2

        def pack_rows(c, carry):
            base = pl.multiple_of(c * chunk, chunk)
            for col in range(2):
                vals = []
                for g in (2 * col, 2 * col + 1):
                    src = pl.ds(g * rows + base, chunk)
                    vals.append(jnp.where(mbuf[q, src, :] != 0, rbuf[q, src, :], jnp.nan))
                x0, x1 = vals
                packed[even, pl.ds(base, chunk), col * 128:(col + 1) * 128] = jnp.where(low_c, x0, pltpu.roll(x1, 64, 1))
                packed[even + 1, pl.ds(base, chunk), col * 128:(col + 1) * 128] = jnp.where(low_c, pltpu.roll(x0, 64, 1), x1)
            return carry

        lax.fori_loop(0, rows // chunk, pack_rows, 0)

    pack_pair(0)

    @pl.when(ships)
    def _():
        ship(0).start()

    def pack_rest(q, carry):
        pack_pair(q)
        return carry

    lax.fori_loop(1, pairs, pack_rest, 0)

    @pl.when(ships)
    def _():
        ship(1).start()

    @pl.when(jnp.logical_and(ships, jnp.logical_not(is_worker)))
    def _():
        def ship_next(k, carry):
            ship(k - 2).wait_send()
            ship(k).start()
            return carry

        lax.fori_loop(2, blk_n, ship_next, 0)
        ship(blk_n - 2).wait_send()
        ship(blk_n - 1).wait_send()

    @pl.when(is_own)
    def _():
        def keep(column, carry):
            work[column, 0] = packed[column]
            return carry

        lax.fori_loop(0, blk_n, keep, 0)
        ut[0] = usrc[...]
        vst[...] = vown[...]

    def halves(q):
        new_half = ut[q].astype(jnp.bfloat16)
        uth[:, q * rows:(q + 1) * rows] = new_half
        uh[q * rows:(q + 1) * rows, :] = new_half.T

    def spread(vp):
        swapped = pltpu.roll(vp, 64, 1)
        full = jnp.concatenate([jnp.where(low, vp, swapped), jnp.where(low, swapped, vp)], axis=0)
        lo = jnp.where(left, full, 0.0).astype(jnp.bfloat16)
        hi = jnp.where(left, 0.0, full).astype(jnp.bfloat16)
        wt[0:rank, 0:128] = lo
        wt[rank:2 * rank, 0:128] = hi
        wt[2 * rank:3 * rank, 128:256] = lo
        wt[3 * rank:4 * rank, 128:256] = hi

    def partial(block):
        for q in range(PIECES):
            sl = slice(q * rows, (q + 1) * rows)
            predicted = jnp.dot(uh[sl, :], wt[...], preferred_element_type=jnp.float32)
            rate = work[block, q]
            err[sl, :] = jnp.where(rate == rate, predicted - rate, 0.0).astype(jnp.bfloat16)
        s = jnp.dot(uth[...], err[...], preferred_element_type=jnp.float32)
        s_lo = s[0:rank, 0:128] + s[2 * rank:3 * rank, 128:256]
        s_hi = s[rank:2 * rank, 0:128] + s[3 * rank:4 * rank, 128:256]
        both = jnp.where(left, s_lo, s_hi)
        top, bottom = both[0:half], both[half:rank]
        return jnp.where(low, top, bottom) + pltpu.roll(jnp.where(low, bottom, top), 64, 1)

    def user_step():
        for q in range(PIECES):
            grad = lax.dot_general(wt[...], err[q * rows:(q + 1) * rows, :], (((1,), (1,)), ((), ())), preferred_element_type=jnp.float32)
            old = ut[q]
            ut[q] = old - step_size * (grad + decay_coef * old)
            halves(q)

    def item_step(parts):
        total = (parts[0] + parts[1]) + (parts[2] + parts[3])
        old = vst[...]
        return old - step_size * (total + decay_coef * old)

    def await_pieces(buf, sem):
        @pl.when(has_own)
        def _():
            most = buf.at[pl.ds(1, PIECES - 1)]
            pltpu.make_async_copy(most, most, sem).wait()

        @pl.when(jnp.logical_not(has_own))
        def _():
            pltpu.make_async_copy(buf, buf, sem).wait()

    def sub_epoch(t, carry):
        block = (job + t) % blk_n

        @pl.when(t < blk_n)
        def _():
            await_pieces(work.at[block], ship_recv.at[block])

        @pl.when(jnp.logical_and(ships, t < blk_n - 2))
        def _():
            ship(t).wait_send()
            ship(t + 2).start()

        for step in range(STEPS - 1):
            spread(vst[...])
            slots[step, place] = partial(block)
            for d in (3, 2, 1):
                pltpu.make_async_remote_copy(
                    src_ref=slots.at[step, place], dst_ref=slots.at[step, place], send_sem=send_sem.at[step], recv_sem=recv_sem.at[step],
                    device_id=worker(job, mate(d)), device_id_type=MESH).start()
            user_step()
            others = slots.at[step, pl.ds(0, TEAM - 1)]
            pltpu.make_async_copy(others, others, send_sem.at[step]).wait()
            pltpu.make_async_copy(others, others, recv_sem.at[step]).wait()
            vst[...] = item_step(slots[step])
        ahead = pltpu.make_async_remote_copy(
            src_ref=vst, dst_ref=vslots.at[t], send_sem=vsend_sem, recv_sem=vrecv_sem.at[t],
            device_id=worker(prev_job, place), device_id_type=MESH)
        ahead.start()
        spread(vst[...])
        xsend[...] = partial(block)
        for d in (3, 2, 1, 0):
            pltpu.make_async_remote_copy(
                src_ref=xsend, dst_ref=xslots.at[t, place], send_sem=xsend_sem, recv_sem=xrecv_sem.at[t],
                device_id=worker(prev_job, mate(d)), device_id_type=MESH).start()
        user_step()
        everyone = xslots.at[t]
        pltpu.make_async_copy(everyone, everyone, xsend_sem).wait()
        ahead.wait()
        pltpu.make_async_copy(everyone, everyone, xrecv_sem.at[t]).wait()
        vst[...] = vslots[t]
        vst[...] = item_step(xslots[t])
        return carry

    def give_users(q):
        return pltpu.make_async_remote_copy(
            src_ref=ut.at[q], dst_ref=uret, send_sem=back_send.at[q], recv_sem=back_recv, device_id=source(q), device_id_type=MESH)

    def give_items(q):
        return pltpu.make_async_remote_copy(
            src_ref=vst, dst_ref=vret, send_sem=final_send.at[q], recv_sem=final_recv, device_id=source(q), device_id_type=MESH)

    @pl.when(is_worker)
    def _():
        wt[...] = jnp.zeros_like(wt)
        await_pieces(ut, user_recv)

        @pl.when(jnp.logical_not(has_own))
        def _():
            pltpu.make_async_copy(vst, vst, item_recv).wait()

        for q in range(PIECES):
            halves(q)
        lax.fori_loop(0, EPOCHS * blk_n, sub_epoch, 0)
        for q in (3, 2, 1):
            give_users(q).start()
            give_items(q).start()

        @pl.when(jnp.logical_not(has_own))
        def _():
            give_users(0).start()
            give_items(0).start()

        @pl.when(ships)
        def _():
            ship(blk_n - 2).wait_send()
            ship(blk_n - 1).wait_send()

    @pl.when(ships)
    def _():
        send_users.wait_send()
        pltpu.make_async_copy(uret, uret, back_recv).wait()
        pltpu.make_async_copy(vret, vret, final_recv).wait()
        for g in range(GROUPS):
            ut_out[:, g * rows:(g + 1) * rows] = uret[g * rank:(g + 1) * rank, :]
        vt_out[0:half, :] = vret[:, 0:64]
        vt_out[half:rank, :] = vret[:, 64:128]

    @pl.when(gives_items)
    def _():
        send_items.wait_send()

    @pl.when(is_own)
    def _():
        for g in range(GROUPS):
            ut_out[:, g * rows:(g + 1) * rows] = ut[0, g * rank:(g + 1) * rank, :]
        vt_out[0:half, :] = vst[:, 0:64]
        vt_out[half:rank, :] = vst[:, 64:128]

    @pl.when(is_worker)
    def _():
        for q in (3, 2, 1):
            give_users(q).wait_send()
            give_items(q).wait_send()

        @pl.when(jnp.logical_not(has_own))
        def _():
            give_users(0).wait_send()
            give_items(0).wait_send()


def solution(mesh):
    blk_n = mesh.shape["blk"]
    sub_n = mesh.shape["sub"]
    row_spec = P(("rep", "blk", "sub"), None)
    item_spec = P(("rep", "blk"), None)

    def local_run(ratings, mask, user_init, item_init):
        users = ratings.shape[0]
        items, rank = item_init.shape
        big_side = max(items, sub_n * users)
        step_size = STEP_GAIN * math.sqrt(rank) / (math.sqrt(big_side) + math.sqrt(rank)) ** 2
        decay_coef = DECAY / step_size
        rows = users // GROUPS
        turns = EPOCHS * blk_n
        half = rank // 2
        wide_u, wide_i = GROUPS * rank, GROUPS * items
        vmem = pl.BlockSpec(memory_space=pltpu.VMEM)
        dma = pltpu.SemaphoreType.DMA
        ut, vt = pl.pallas_call(
            functools.partial(kernel, (blk_n, step_size, decay_coef)),
            out_shape=(jax.ShapeDtypeStruct((rank, users), jnp.float32), jax.ShapeDtypeStruct((rank, items), jnp.float32)),
            in_specs=[pl.BlockSpec(memory_space=pl.ANY)] * 4,
            out_specs=(vmem, vmem),
            scratch_shapes=[
                pltpu.VMEM((blk_n // 2, users, 128), jnp.float32),
                pltpu.VMEM((blk_n // 2, users, 128), jnp.int32),
                pltpu.VMEM((rank, users), jnp.float32),
                pltpu.VMEM((rank, items), jnp.float32),
                pltpu.VMEM((blk_n, rows, wide_i), jnp.float32),
                pltpu.VMEM((blk_n, PIECES, rows, wide_i), jnp.float32),
                pltpu.VMEM((wide_u, rows), jnp.float32),
                pltpu.VMEM((wide_u, rows), jnp.float32),
                pltpu.VMEM((half, 128), jnp.float32),
                pltpu.VMEM((half, 128), jnp.float32),
                pltpu.VMEM((PIECES, wide_u, rows), jnp.float32),
                pltpu.VMEM((PIECES * rows, wide_u), jnp.bfloat16),
                pltpu.VMEM((wide_u, PIECES * rows), jnp.bfloat16),
                pltpu.VMEM((wide_u, wide_i), jnp.bfloat16),
                pltpu.VMEM((PIECES * rows, wide_i), jnp.bfloat16),
                pltpu.VMEM((half, 128), jnp.float32),
                pltpu.VMEM((half, 128), jnp.float32),
                pltpu.VMEM((STEPS - 1, TEAM, half, 128), jnp.float32),
                pltpu.VMEM((turns, TEAM, half, 128), jnp.float32),
                pltpu.VMEM((turns, half, 128), jnp.float32),
                dma((3, blk_n // 2)),
                dma((blk_n,)), dma((blk_n,)),
                dma, dma, dma, dma,
                dma((PIECES,)), dma,
                dma((PIECES,)), dma,
                dma((STEPS - 1,)), dma((STEPS - 1,)),
                dma, dma((turns,)),
                dma, dma((turns,)),
            ],
            compiler_params=pltpu.CompilerParams(collective_id=0, has_side_effects=True, vmem_limit_bytes=67043328),
        )(ratings, mask, user_init.T, item_init.T)
        return ut.T, vt.T

    return jax.shard_map(local_run, mesh=mesh, in_specs=(row_spec, row_spec, row_spec, item_spec), out_specs=(row_spec, item_spec), check_vma=False)
```

```python
import functools
import math

import jax
import jax.numpy as jnp
from jax import lax
from jax.experimental import pallas as pl
from jax.experimental.pallas import tpu as pltpu
from jax.sharding import PartitionSpec as P

STEPS = 4
EPOCHS = 2
STEP_GAIN = 0.4
DECAY = 0.002
GROUPS = 4
TEAM = 4
PIECES = 4
MESH = pl.DeviceIdType.MESH


def kernel(dims, r_hbm, m_hbm, u_hbm, v_hbm, ut_out, vt_out, rbuf, mbuf, ubuf, vbuf, packed, work, usrc, uret, vown, vret, ut, uh, uth, wt, err, vst,
           xsend, slots, xslots, vslots, load_sem, ship_send, ship_recv, user_send, user_recv, item_send, item_recv, back_send, back_recv,
           final_send, final_recv, send_sem, recv_sem, xsend_sem, xrecv_sem, vsend_sem, vrecv_sem, credit):
    blk_n, step_size, decay_coef = dims
    rank, users = ubuf.shape
    rows = users // GROUPS
    half = rank // 2
    pairs = blk_n // 2
    me_b = lax.axis_index("blk")
    me_s = lax.axis_index("sub")
    x, core = me_b // 2, me_b % 2
    z, y = me_s // 4, me_s % 4

    out_y = (y // 2 + core + x) % 2
    out_z = z // 2
    piece = 2 * out_y + out_z
    target = {"sub": (z + out_z * (3 - 2 * z)) * 4 + y + out_y * (3 - 2 * y), "blk": 2 * x + 1}
    is_own = jnp.logical_and(core == 1, piece == 0)
    ships = jnp.logical_not(is_own)
    is_worker = jnp.logical_and(core == 1, z < 2)
    job_core = (y // 2 + x) % 2
    job = 2 * x + job_core
    has_own = job_core == 1
    place = (z % 2) * 2 + y % 2

    def source(q):
        oy, oz = q // 2, q % 2
        return {"sub": (z + oz * (3 - 2 * z)) * 4 + y + oy * (3 - 2 * y), "blk": job}

    def worker(block, p):
        bx = block // 2
        return {"sub": (p // 2) * 4 + 2 * ((block % 2 + bx) % 2) + p % 2, "blk": 2 * bx + 1}

    prev_job = (job + blk_n - 1) % blk_n
    next_job = (job + 1) % blk_n

    def mate(d):
        dz, dy = d // 2, d % 2
        pz, py = (place // 2 + dz) % 2, (place % 2 + dy) % 2
        return pz * 2 + py

    def load(q, src, dst, kind):
        col = pl.multiple_of(((x + q) % pairs) * 128, 128)
        return pltpu.make_async_copy(src.at[:, pl.ds(col, 128)], dst.at[q], load_sem.at[kind, q])

    load_users = pltpu.make_async_copy(u_hbm, ubuf, load_sem.at[2, 0])
    load_items = pltpu.make_async_copy(v_hbm, vbuf, load_sem.at[2, 1])
    load_users.start()
    load_items.start()
    for q in range(pairs):
        load(q, r_hbm, rbuf, 0).start()
        load(q, m_hbm, mbuf, 1).start()

    barrier = pltpu.get_barrier_semaphore()

    def greet(device):
        pl.semaphore_signal(barrier, inc=1, device_id=device, device_id_type=MESH)

    @pl.when(ships)
    def _():
        greet(target)

    @pl.when(is_worker)
    def _():
        for q in range(1, PIECES):
            greet(source(q))

        @pl.when(jnp.logical_not(has_own))
        def _():
            greet(source(0))

        for d in (3, 2, 1):
            greet(worker(job, mate(d)))
        for p in range(TEAM):
            greet(worker(prev_job, p))
            greet(worker(next_job, p))

    low = lax.broadcasted_iota(jnp.int32, (half, 128), 1) < 64
    left = lax.broadcasted_iota(jnp.int32, (rank, 128), 1) < 64

    load_users.wait()
    for g in range(GROUPS):
        usrc[g * rank:(g + 1) * rank, :] = ubuf[:, g * rows:(g + 1) * rows]
    load_items.wait()
    vown[:, 0:64] = vbuf[0:half, :]
    vown[:, 64:128] = vbuf[half:rank, :]

    @pl.when(jnp.logical_not(is_worker))
    def _():
        pl.semaphore_wait(barrier, 1)

    @pl.when(jnp.logical_and(is_worker, has_own))
    def _():
        pl.semaphore_wait(barrier, PIECES - 1 + TEAM - 1 + 2 * TEAM)

    @pl.when(jnp.logical_and(is_worker, jnp.logical_not(has_own)))
    def _():
        pl.semaphore_wait(barrier, PIECES + 1 + TEAM - 1 + 2 * TEAM)

    send_users = pltpu.make_async_remote_copy(
        src_ref=usrc, dst_ref=ut.at[piece], send_sem=user_send, recv_sem=user_recv, device_id=target, device_id_type=MESH)
    send_items = pltpu.make_async_remote_copy(
        src_ref=vown, dst_ref=vst, send_sem=item_send, recv_sem=item_recv, device_id=target, device_id_type=MESH)
    gives_items = jnp.logical_and(core == 0, piece == 0)

    @pl.when(ships)
    def _():
        send_users.start()

    @pl.when(gives_items)
    def _():
        send_items.start()

    def ship(k):
        column = (me_b + k) % blk_n
        return pltpu.make_async_remote_copy(
            src_ref=packed.at[column], dst_ref=work.at[column, piece], send_sem=ship_send.at[k], recv_sem=ship_recv.at[column],
            device_id=target, device_id_type=MESH)

    chunk = 64
    low_c = lax.broadcasted_iota(jnp.int32, (chunk, 128), 1) < 64

    def pack_pair(q):
        load(q, r_hbm, rbuf, 0).wait()
        load(q, m_hbm, mbuf, 1).wait()
        even = ((x + q) % pairs) * 2

        def pack_rows(c, carry):
            base = pl.multiple_of(c * chunk, chunk)
            for col in range(2):
                vals = []
                for g in (2 * col, 2 * col + 1):
                    src = pl.ds(g * rows + base, chunk)
                    vals.append(jnp.where(mbuf[q, src, :] != 0, rbuf[q, src, :], jnp.nan))
                x0, x1 = vals
                packed[even, pl.ds(base, chunk), col * 128:(col + 1) * 128] = jnp.where(low_c, x0, pltpu.roll(x1, 64, 1))
                packed[even + 1, pl.ds(base, chunk), col * 128:(col + 1) * 128] = jnp.where(low_c, pltpu.roll(x0, 64, 1), x1)
            return carry

        lax.fori_loop(0, rows // chunk, pack_rows, 0)

    pack_pair(0)

    @pl.when(ships)
    def _():
        ship(0).start()

    def pack_rest(q, carry):
        pack_pair(q)
        return carry

    lax.fori_loop(1, pairs, pack_rest, 0)

    is_far = piece == 3

    @pl.when(is_far)
    def _():
        def ship_far(k, carry):
            pl.semaphore_wait(credit, 1)
            ship(k).start()
            ship(k - 1).wait_send()
            return carry

        lax.fori_loop(1, blk_n, ship_far, 0)
        ship(blk_n - 1).wait_send()

    @pl.when(jnp.logical_and(ships, jnp.logical_not(is_far)))
    def _():
        ship(1).start()

    @pl.when(jnp.logical_and(ships, jnp.logical_not(jnp.logical_or(is_worker, is_far))))
    def _():
        def ship_next(k, carry):
            ship(k - 2).wait_send()
            ship(k).start()
            return carry

        lax.fori_loop(2, blk_n, ship_next, 0)
        ship(blk_n - 2).wait_send()
        ship(blk_n - 1).wait_send()

    @pl.when(is_own)
    def _():
        def keep(column, carry):
            work[column, 0] = packed[column]
            return carry

        lax.fori_loop(0, blk_n, keep, 0)
        ut[0] = usrc[...]
        vst[...] = vown[...]

    def halves(q):
        new_half = ut[q].astype(jnp.bfloat16)
        uth[:, q * rows:(q + 1) * rows] = new_half
        uh[q * rows:(q + 1) * rows, :] = new_half.T

    def spread(vp):
        swapped = pltpu.roll(vp, 64, 1)
        full = jnp.concatenate([jnp.where(low, vp, swapped), jnp.where(low, swapped, vp)], axis=0)
        lo = jnp.where(left, full, 0.0).astype(jnp.bfloat16)
        hi = jnp.where(left, 0.0, full).astype(jnp.bfloat16)
        wt[0:rank, 0:128] = lo
        wt[rank:2 * rank, 0:128] = hi
        wt[2 * rank:3 * rank, 128:256] = lo
        wt[3 * rank:4 * rank, 128:256] = hi

    def partial(block):
        for q in range(PIECES):
            sl = slice(q * rows, (q + 1) * rows)
            predicted = jnp.dot(uh[sl, :], wt[...], preferred_element_type=jnp.float32)
            rate = work[block, q]
            err[sl, :] = jnp.where(rate == rate, predicted - rate, 0.0).astype(jnp.bfloat16)
        s = jnp.dot(uth[...], err[...], preferred_element_type=jnp.float32)
        s_lo = s[0:rank, 0:128] + s[2 * rank:3 * rank, 128:256]
        s_hi = s[rank:2 * rank, 0:128] + s[3 * rank:4 * rank, 128:256]
        both = jnp.where(left, s_lo, s_hi)
        top, bottom = both[0:half], both[half:rank]
        return jnp.where(low, top, bottom) + pltpu.roll(jnp.where(low, bottom, top), 64, 1)

    def user_step():
        for q in range(PIECES):
            grad = lax.dot_general(wt[...], err[q * rows:(q + 1) * rows, :], (((1,), (1,)), ((), ())), preferred_element_type=jnp.float32)
            old = ut[q]
            ut[q] = old - step_size * (grad + decay_coef * old)
            halves(q)

    def item_step(parts):
        total = (parts[0] + parts[1]) + (parts[2] + parts[3])
        old = vst[...]
        return old - step_size * (total + decay_coef * old)

    def await_pieces(buf, sem):
        @pl.when(has_own)
        def _():
            most = buf.at[pl.ds(1, PIECES - 1)]
            pltpu.make_async_copy(most, most, sem).wait()

        @pl.when(jnp.logical_not(has_own))
        def _():
            pltpu.make_async_copy(buf, buf, sem).wait()

    def sub_epoch(t, carry):
        block = (job + t) % blk_n

        @pl.when(t < blk_n)
        def _():
            await_pieces(work.at[block], ship_recv.at[block])

        @pl.when(t < blk_n - 1)
        def _():
            pl.semaphore_signal(credit, inc=1, device_id=source(3), device_id_type=MESH)

        @pl.when(jnp.logical_and(ships, t < blk_n - 2))
        def _():
            ship(t).wait_send()
            ship(t + 2).start()

        for step in range(STEPS - 1):
            spread(vst[...])
            slots[step, place] = partial(block)
            for d in (3, 2, 1):
                pltpu.make_async_remote_copy(
                    src_ref=slots.at[step, place], dst_ref=slots.at[step, place], send_sem=send_sem.at[step], recv_sem=recv_sem.at[step],
                    device_id=worker(job, mate(d)), device_id_type=MESH).start()
            user_step()
            others = slots.at[step, pl.ds(0, TEAM - 1)]
            pltpu.make_async_copy(others, others, send_sem.at[step]).wait()
            pltpu.make_async_copy(others, others, recv_sem.at[step]).wait()
            vst[...] = item_step(slots[step])
        ahead = pltpu.make_async_remote_copy(
            src_ref=vst, dst_ref=vslots.at[t], send_sem=vsend_sem, recv_sem=vrecv_sem.at[t],
            device_id=worker(prev_job, place), device_id_type=MESH)
        ahead.start()
        spread(vst[...])
        xsend[...] = partial(block)
        for d in (3, 2, 1, 0):
            pltpu.make_async_remote_copy(
                src_ref=xsend, dst_ref=xslots.at[t, place], send_sem=xsend_sem, recv_sem=xrecv_sem.at[t],
                device_id=worker(prev_job, mate(d)), device_id_type=MESH).start()
        user_step()
        everyone = xslots.at[t]
        pltpu.make_async_copy(everyone, everyone, xsend_sem).wait()
        ahead.wait()
        pltpu.make_async_copy(everyone, everyone, xrecv_sem.at[t]).wait()
        vst[...] = vslots[t]
        vst[...] = item_step(xslots[t])
        return carry

    def give_users(q):
        return pltpu.make_async_remote_copy(
            src_ref=ut.at[q], dst_ref=uret, send_sem=back_send.at[q], recv_sem=back_recv, device_id=source(q), device_id_type=MESH)

    def give_items(q):
        return pltpu.make_async_remote_copy(
            src_ref=vst, dst_ref=vret, send_sem=final_send.at[q], recv_sem=final_recv, device_id=source(q), device_id_type=MESH)

    @pl.when(is_worker)
    def _():
        wt[...] = jnp.zeros_like(wt)
        await_pieces(ut, user_recv)

        @pl.when(jnp.logical_not(has_own))
        def _():
            pltpu.make_async_copy(vst, vst, item_recv).wait()

        for q in range(PIECES):
            halves(q)
        lax.fori_loop(0, EPOCHS * blk_n, sub_epoch, 0)
        for q in (3, 2, 1):
            give_users(q).start()
            give_items(q).start()

        @pl.when(jnp.logical_not(has_own))
        def _():
            give_users(0).start()
            give_items(0).start()

        @pl.when(ships)
        def _():
            ship(blk_n - 2).wait_send()
            ship(blk_n - 1).wait_send()

    @pl.when(ships)
    def _():
        send_users.wait_send()
        pltpu.make_async_copy(uret, uret, back_recv).wait()
        pltpu.make_async_copy(vret, vret, final_recv).wait()
        for g in range(GROUPS):
            ut_out[:, g * rows:(g + 1) * rows] = uret[g * rank:(g + 1) * rank, :]
        vt_out[0:half, :] = vret[:, 0:64]
        vt_out[half:rank, :] = vret[:, 64:128]

    @pl.when(gives_items)
    def _():
        send_items.wait_send()

    @pl.when(is_own)
    def _():
        for g in range(GROUPS):
            ut_out[:, g * rows:(g + 1) * rows] = ut[0, g * rank:(g + 1) * rank, :]
        vt_out[0:half, :] = vst[:, 0:64]
        vt_out[half:rank, :] = vst[:, 64:128]

    @pl.when(is_worker)
    def _():
        for q in (3, 2, 1):
            give_users(q).wait_send()
            give_items(q).wait_send()

        @pl.when(jnp.logical_not(has_own))
        def _():
            give_users(0).wait_send()
            give_items(0).wait_send()


def solution(mesh):
    blk_n = mesh.shape["blk"]
    sub_n = mesh.shape["sub"]
    row_spec = P(("rep", "blk", "sub"), None)
    item_spec = P(("rep", "blk"), None)

    def local_run(ratings, mask, user_init, item_init):
        users = ratings.shape[0]
        items, rank = item_init.shape
        big_side = max(items, sub_n * users)
        step_size = STEP_GAIN * math.sqrt(rank) / (math.sqrt(big_side) + math.sqrt(rank)) ** 2
        decay_coef = DECAY / step_size
        rows = users // GROUPS
        turns = EPOCHS * blk_n
        half = rank // 2
        wide_u, wide_i = GROUPS * rank, GROUPS * items
        vmem = pl.BlockSpec(memory_space=pltpu.VMEM)
        dma = pltpu.SemaphoreType.DMA
        ut, vt = pl.pallas_call(
            functools.partial(kernel, (blk_n, step_size, decay_coef)),
            out_shape=(jax.ShapeDtypeStruct((rank, users), jnp.float32), jax.ShapeDtypeStruct((rank, items), jnp.float32)),
            in_specs=[pl.BlockSpec(memory_space=pl.ANY)] * 4,
            out_specs=(vmem, vmem),
            scratch_shapes=[
                pltpu.VMEM((blk_n // 2, users, 128), jnp.float32),
                pltpu.VMEM((blk_n // 2, users, 128), jnp.int32),
                pltpu.VMEM((rank, users), jnp.float32),
                pltpu.VMEM((rank, items), jnp.float32),
                pltpu.VMEM((blk_n, rows, wide_i), jnp.float32),
                pltpu.VMEM((blk_n, PIECES, rows, wide_i), jnp.float32),
                pltpu.VMEM((wide_u, rows), jnp.float32),
                pltpu.VMEM((wide_u, rows), jnp.float32),
                pltpu.VMEM((half, 128), jnp.float32),
                pltpu.VMEM((half, 128), jnp.float32),
                pltpu.VMEM((PIECES, wide_u, rows), jnp.float32),
                pltpu.VMEM((PIECES * rows, wide_u), jnp.bfloat16),
                pltpu.VMEM((wide_u, PIECES * rows), jnp.bfloat16),
                pltpu.VMEM((wide_u, wide_i), jnp.bfloat16),
                pltpu.VMEM((PIECES * rows, wide_i), jnp.bfloat16),
                pltpu.VMEM((half, 128), jnp.float32),
                pltpu.VMEM((half, 128), jnp.float32),
                pltpu.VMEM((STEPS - 1, TEAM, half, 128), jnp.float32),
                pltpu.VMEM((turns, TEAM, half, 128), jnp.float32),
                pltpu.VMEM((turns, half, 128), jnp.float32),
                dma((3, blk_n // 2)),
                dma((blk_n,)), dma((blk_n,)),
                dma, dma, dma, dma,
                dma((PIECES,)), dma,
                dma((PIECES,)), dma,
                dma((STEPS - 1,)), dma((STEPS - 1,)),
                dma, dma((turns,)),
                dma, dma((turns,)),
                pltpu.SemaphoreType.REGULAR,
            ],
            compiler_params=pltpu.CompilerParams(collective_id=0, has_side_effects=True, vmem_limit_bytes=67043328),
        )(ratings, mask, user_init.T, item_init.T)
        return ut.T, vt.T

    return jax.shard_map(local_run, mesh=mesh, in_specs=(row_spec, row_spec, row_spec, item_spec), out_specs=(row_spec, item_spec), check_vma=False)
```

```python
import functools
import math

import jax
import jax.numpy as jnp
from jax import lax
from jax.experimental import pallas as pl
from jax.experimental.pallas import tpu as pltpu
from jax.sharding import PartitionSpec as P

STEPS = 4
EPOCHS = 2
STEP_GAIN = 0.4
DECAY = 0.002
GROUPS = 4
TEAM = 4
PIECES = 4
MESH = pl.DeviceIdType.MESH


def kernel(dims, r_hbm, m_hbm, u_hbm, v_hbm, ut_out, vt_out, rbuf, mbuf, ubuf, vbuf, packed, work, usrc, uret, vown, vret, ut, uh, uth, wt, err, vst,
           xsend, slots, xslots, vslots, load_sem, ship_send, ship_recv, user_send, user_recv, item_send, item_recv, back_send, back_recv,
           final_send, final_recv, send_sem, recv_sem, xsend_sem, xrecv_sem, vsend_sem, vrecv_sem, credit):
    blk_n, step_size, decay_coef = dims
    rank, users = ubuf.shape
    rows = users // GROUPS
    half = rank // 2
    pairs = blk_n // 2
    me_b = lax.axis_index("blk")
    me_s = lax.axis_index("sub")
    x, core = me_b // 2, me_b % 2
    z, y = me_s // 4, me_s % 4

    out_y = (y // 2 + core + x) % 2
    out_z = z // 2
    piece = 2 * out_y + out_z
    target = {"sub": (z + out_z * (3 - 2 * z)) * 4 + y + out_y * (3 - 2 * y), "blk": 2 * x + 1}
    is_own = jnp.logical_and(core == 1, piece == 0)
    ships = jnp.logical_not(is_own)
    is_worker = jnp.logical_and(core == 1, z < 2)
    job_core = (y // 2 + x) % 2
    job = 2 * x + job_core
    has_own = job_core == 1
    place = (z % 2) * 2 + y % 2

    def source(q):
        oy, oz = q // 2, q % 2
        return {"sub": (z + oz * (3 - 2 * z)) * 4 + y + oy * (3 - 2 * y), "blk": job}

    def worker(block, p):
        bx = block // 2
        return {"sub": (p // 2) * 4 + 2 * ((block % 2 + bx) % 2) + p % 2, "blk": 2 * bx + 1}

    prev_job = (job + blk_n - 1) % blk_n
    next_job = (job + 1) % blk_n

    def mate(d, flip=0):
        dz, dy = d // 2, d % 2
        pz, py = (place // 2 + dz) % 2, (place % 2 + dy + flip) % 2
        return pz * 2 + py

    def load(q, src, dst, kind):
        col = pl.multiple_of(((x + q) % pairs) * 128, 128)
        return pltpu.make_async_copy(src.at[:, pl.ds(col, 128)], dst.at[q], load_sem.at[kind, q])

    load_users = pltpu.make_async_copy(u_hbm, ubuf, load_sem.at[2, 0])
    load_items = pltpu.make_async_copy(v_hbm, vbuf, load_sem.at[2, 1])
    load_users.start()
    load_items.start()
    load(0, r_hbm, rbuf, 0).start()
    load(0, m_hbm, mbuf, 1).start()

    barrier = pltpu.get_barrier_semaphore()

    def greet(device):
        pl.semaphore_signal(barrier, inc=1, device_id=device, device_id_type=MESH)

    @pl.when(ships)
    def _():
        greet(target)

    @pl.when(is_worker)
    def _():
        for q in range(1, PIECES):
            greet(source(q))

        @pl.when(jnp.logical_not(has_own))
        def _():
            greet(source(0))

        for d in (3, 2, 1):
            greet(worker(job, mate(d)))
        for p in range(TEAM):
            greet(worker(prev_job, p))
            greet(worker(next_job, p))

    low = lax.broadcasted_iota(jnp.int32, (half, 128), 1) < 64
    left = lax.broadcasted_iota(jnp.int32, (rank, 128), 1) < 64

    load(0, r_hbm, rbuf, 0).wait()
    load(0, m_hbm, mbuf, 1).wait()
    for q in range(1, pairs):
        load(q, r_hbm, rbuf, 0).start()
        load(q, m_hbm, mbuf, 1).start()
    load_users.wait()
    for g in range(GROUPS):
        usrc[g * rank:(g + 1) * rank, :] = ubuf[:, g * rows:(g + 1) * rows]
    load_items.wait()
    vown[:, 0:64] = vbuf[0:half, :]
    vown[:, 64:128] = vbuf[half:rank, :]

    @pl.when(jnp.logical_not(is_worker))
    def _():
        pl.semaphore_wait(barrier, 1)

    @pl.when(jnp.logical_and(is_worker, has_own))
    def _():
        pl.semaphore_wait(barrier, PIECES - 1 + TEAM - 1 + 2 * TEAM)

    @pl.when(jnp.logical_and(is_worker, jnp.logical_not(has_own)))
    def _():
        pl.semaphore_wait(barrier, PIECES + 1 + TEAM - 1 + 2 * TEAM)

    send_users = pltpu.make_async_remote_copy(
        src_ref=usrc, dst_ref=ut.at[piece], send_sem=user_send, recv_sem=user_recv, device_id=target, device_id_type=MESH)
    send_items = pltpu.make_async_remote_copy(
        src_ref=vown, dst_ref=vst, send_sem=item_send, recv_sem=item_recv, device_id=target, device_id_type=MESH)
    gives_items = jnp.logical_and(core == 0, piece == 0)

    @pl.when(ships)
    def _():
        send_users.start()

    @pl.when(gives_items)
    def _():
        send_items.start()

    def ship(k):
        column = (me_b + k) % blk_n
        return pltpu.make_async_remote_copy(
            src_ref=packed.at[column], dst_ref=work.at[column, piece], send_sem=ship_send.at[k], recv_sem=ship_recv.at[column],
            device_id=target, device_id_type=MESH)

    chunk = 64
    low_c = lax.broadcasted_iota(jnp.int32, (chunk, 128), 1) < 64

    def pack_pair(q):
        even = ((x + q) % pairs) * 2

        def pack_rows(c, carry):
            base = pl.multiple_of(c * chunk, chunk)
            for col in range(2):
                vals = []
                for g in (2 * col, 2 * col + 1):
                    src = pl.ds(g * rows + base, chunk)
                    vals.append(jnp.where(mbuf[q, src, :] != 0, rbuf[q, src, :], jnp.nan))
                x0, x1 = vals
                packed[even, pl.ds(base, chunk), col * 128:(col + 1) * 128] = jnp.where(low_c, x0, pltpu.roll(x1, 64, 1))
                packed[even + 1, pl.ds(base, chunk), col * 128:(col + 1) * 128] = jnp.where(low_c, pltpu.roll(x0, 64, 1), x1)
            return carry

        lax.fori_loop(0, rows // chunk, pack_rows, 0)

    pack_pair(0)

    @pl.when(ships)
    def _():
        ship(0).start()

    def pack_rest(q, carry):
        load(q, r_hbm, rbuf, 0).wait()
        load(q, m_hbm, mbuf, 1).wait()
        pack_pair(q)
        return carry

    lax.fori_loop(1, pairs, pack_rest, 0)

    is_far = piece == 3

    @pl.when(is_far)
    def _():
        def ship_far(k, carry):
            pl.semaphore_wait(credit, 1)
            ship(k).start()
            ship(k - 1).wait_send()
            return carry

        lax.fori_loop(1, blk_n, ship_far, 0)
        ship(blk_n - 1).wait_send()

    @pl.when(jnp.logical_and(ships, jnp.logical_not(is_far)))
    def _():
        ship(1).start()

    @pl.when(jnp.logical_and(ships, jnp.logical_not(jnp.logical_or(is_worker, is_far))))
    def _():
        def ship_next(k, carry):
            ship(k - 2).wait_send()
            ship(k).start()
            return carry

        lax.fori_loop(2, blk_n, ship_next, 0)
        ship(blk_n - 2).wait_send()
        ship(blk_n - 1).wait_send()

    @pl.when(is_own)
    def _():
        def keep(column, carry):
            work[column, 0] = packed[column]
            return carry

        lax.fori_loop(0, blk_n, keep, 0)
        ut[0] = usrc[...]
        vst[...] = vown[...]

    def halves(q):
        new_half = ut[q].astype(jnp.bfloat16)
        uth[:, q * rows:(q + 1) * rows] = new_half
        uh[q * rows:(q + 1) * rows, :] = new_half.T

    def spread(vp):
        swapped = pltpu.roll(vp, 64, 1)
        full = jnp.concatenate([jnp.where(low, vp, swapped), jnp.where(low, swapped, vp)], axis=0)
        lo = jnp.where(left, full, 0.0).astype(jnp.bfloat16)
        hi = jnp.where(left, 0.0, full).astype(jnp.bfloat16)
        wt[0:rank, 0:128] = lo
        wt[rank:2 * rank, 0:128] = hi
        wt[2 * rank:3 * rank, 128:256] = lo
        wt[3 * rank:4 * rank, 128:256] = hi

    def partial(block):
        for q in range(PIECES):
            sl = slice(q * rows, (q + 1) * rows)
            predicted = jnp.dot(uh[sl, :], wt[...], preferred_element_type=jnp.float32)
            rate = work[block, q]
            err[sl, :] = jnp.where(rate == rate, predicted - rate, 0.0).astype(jnp.bfloat16)
        s = jnp.dot(uth[...], err[...], preferred_element_type=jnp.float32)
        s_lo = s[0:rank, 0:128] + s[2 * rank:3 * rank, 128:256]
        s_hi = s[rank:2 * rank, 0:128] + s[3 * rank:4 * rank, 128:256]
        both = jnp.where(left, s_lo, s_hi)
        top, bottom = both[0:half], both[half:rank]
        return jnp.where(low, top, bottom) + pltpu.roll(jnp.where(low, bottom, top), 64, 1)

    def user_step():
        for q in range(PIECES):
            grad = lax.dot_general(wt[...], err[q * rows:(q + 1) * rows, :], (((1,), (1,)), ((), ())), preferred_element_type=jnp.float32)
            old = ut[q]
            ut[q] = old - step_size * (grad + decay_coef * old)
            halves(q)

    def item_step(parts):
        total = (parts[0] + parts[1]) + (parts[2] + parts[3])
        old = vst[...]
        return old - step_size * (total + decay_coef * old)

    def await_pieces(buf, sem):
        @pl.when(has_own)
        def _():
            most = buf.at[pl.ds(1, PIECES - 1)]
            pltpu.make_async_copy(most, most, sem).wait()

        @pl.when(jnp.logical_not(has_own))
        def _():
            pltpu.make_async_copy(buf, buf, sem).wait()

    def give_users(q):
        return pltpu.make_async_remote_copy(
            src_ref=ut.at[q], dst_ref=uret, send_sem=back_send.at[q], recv_sem=back_recv, device_id=source(q), device_id_type=MESH)

    def give_items(q):
        return pltpu.make_async_remote_copy(
            src_ref=vst, dst_ref=vret, send_sem=final_send.at[q], recv_sem=final_recv, device_id=source(q), device_id_type=MESH)

    def sub_epoch(t, carry):
        block = (job + t) % blk_n

        @pl.when(t < blk_n)
        def _():
            await_pieces(work.at[block], ship_recv.at[block])

        @pl.when(t < blk_n - 1)
        def _():
            pl.semaphore_signal(credit, inc=1, device_id=source(3), device_id_type=MESH)

        @pl.when(jnp.logical_and(ships, t < blk_n - 2))
        def _():
            ship(t).wait_send()
            ship(t + 2).start()

        for step in range(STEPS - 1):
            spread(vst[...])
            slots[step, place] = partial(block)
            for d in (3, 2, 1):
                pltpu.make_async_remote_copy(
                    src_ref=slots.at[step, place], dst_ref=slots.at[step, place], send_sem=send_sem.at[step], recv_sem=recv_sem.at[step],
                    device_id=worker(job, mate(d)), device_id_type=MESH).start()
            user_step()
            others = slots.at[step, pl.ds(0, TEAM - 1)]
            pltpu.make_async_copy(others, others, send_sem.at[step]).wait()
            pltpu.make_async_copy(others, others, recv_sem.at[step]).wait()
            vst[...] = item_step(slots[step])
        ahead = pltpu.make_async_remote_copy(
            src_ref=vst, dst_ref=vslots.at[t], send_sem=vsend_sem, recv_sem=vrecv_sem.at[t],
            device_id=worker(prev_job, place), device_id_type=MESH)
        ahead.start()
        spread(vst[...])
        xsend[...] = partial(block)
        for d in (3, 2, 1, 0):
            pltpu.make_async_remote_copy(
                src_ref=xsend, dst_ref=xslots.at[t, place], send_sem=xsend_sem, recv_sem=xrecv_sem.at[t],
                device_id=worker(prev_job, mate(d, job_core)), device_id_type=MESH).start()
        user_step()

        @pl.when(t == EPOCHS * blk_n - 1)
        def _():
            for q in (3, 1, 2):
                give_users(q).start()

            @pl.when(jnp.logical_not(has_own))
            def _():
                give_users(0).start()

        everyone = xslots.at[t]
        pltpu.make_async_copy(everyone, everyone, xsend_sem).wait()
        ahead.wait()
        pltpu.make_async_copy(everyone, everyone, xrecv_sem.at[t]).wait()
        vst[...] = vslots[t]
        vst[...] = item_step(xslots[t])
        return carry

    @pl.when(is_worker)
    def _():
        wt[...] = jnp.zeros_like(wt)
        await_pieces(ut, user_recv)

        @pl.when(jnp.logical_not(has_own))
        def _():
            pltpu.make_async_copy(vst, vst, item_recv).wait()

        for q in range(PIECES):
            halves(q)
        lax.fori_loop(0, EPOCHS * blk_n, sub_epoch, 0)
        for q in (3, 2, 1):
            give_items(q).start()

        @pl.when(jnp.logical_not(has_own))
        def _():
            give_items(0).start()

        @pl.when(ships)
        def _():
            ship(blk_n - 2).wait_send()
            ship(blk_n - 1).wait_send()

    @pl.when(ships)
    def _():
        send_users.wait_send()
        pltpu.make_async_copy(uret, uret, back_recv).wait()
        pltpu.make_async_copy(vret, vret, final_recv).wait()
        for g in range(GROUPS):
            ut_out[:, g * rows:(g + 1) * rows] = uret[g * rank:(g + 1) * rank, :]
        vt_out[0:half, :] = vret[:, 0:64]
        vt_out[half:rank, :] = vret[:, 64:128]

    @pl.when(gives_items)
    def _():
        send_items.wait_send()

    @pl.when(is_own)
    def _():
        for g in range(GROUPS):
            ut_out[:, g * rows:(g + 1) * rows] = ut[0, g * rank:(g + 1) * rank, :]
        vt_out[0:half, :] = vst[:, 0:64]
        vt_out[half:rank, :] = vst[:, 64:128]

    @pl.when(is_worker)
    def _():
        for q in (3, 2, 1):
            give_users(q).wait_send()
            give_items(q).wait_send()

        @pl.when(jnp.logical_not(has_own))
        def _():
            give_users(0).wait_send()
            give_items(0).wait_send()


def solution(mesh):
    blk_n = mesh.shape["blk"]
    sub_n = mesh.shape["sub"]
    row_spec = P(("rep", "blk", "sub"), None)
    item_spec = P(("rep", "blk"), None)

    def local_run(ratings, mask, user_init, item_init):
        users = ratings.shape[0]
        items, rank = item_init.shape
        big_side = max(items, sub_n * users)
        step_size = STEP_GAIN * math.sqrt(rank) / (math.sqrt(big_side) + math.sqrt(rank)) ** 2
        decay_coef = DECAY / step_size
        rows = users // GROUPS
        turns = EPOCHS * blk_n
        half = rank // 2
        wide_u, wide_i = GROUPS * rank, GROUPS * items
        vmem = pl.BlockSpec(memory_space=pltpu.VMEM)
        dma = pltpu.SemaphoreType.DMA
        ut, vt = pl.pallas_call(
            functools.partial(kernel, (blk_n, step_size, decay_coef)),
            out_shape=(jax.ShapeDtypeStruct((rank, users), jnp.float32), jax.ShapeDtypeStruct((rank, items), jnp.float32)),
            in_specs=[pl.BlockSpec(memory_space=pl.ANY)] * 4,
            out_specs=(vmem, vmem),
            scratch_shapes=[
                pltpu.VMEM((blk_n // 2, users, 128), jnp.float32),
                pltpu.VMEM((blk_n // 2, users, 128), jnp.int32),
                pltpu.VMEM((rank, users), jnp.float32),
                pltpu.VMEM((rank, items), jnp.float32),
                pltpu.VMEM((blk_n, rows, wide_i), jnp.float32),
                pltpu.VMEM((blk_n, PIECES, rows, wide_i), jnp.float32),
                pltpu.VMEM((wide_u, rows), jnp.float32),
                pltpu.VMEM((wide_u, rows), jnp.float32),
                pltpu.VMEM((half, 128), jnp.float32),
                pltpu.VMEM((half, 128), jnp.float32),
                pltpu.VMEM((PIECES, wide_u, rows), jnp.float32),
                pltpu.VMEM((PIECES * rows, wide_u), jnp.bfloat16),
                pltpu.VMEM((wide_u, PIECES * rows), jnp.bfloat16),
                pltpu.VMEM((wide_u, wide_i), jnp.bfloat16),
                pltpu.VMEM((PIECES * rows, wide_i), jnp.bfloat16),
                pltpu.VMEM((half, 128), jnp.float32),
                pltpu.VMEM((half, 128), jnp.float32),
                pltpu.VMEM((STEPS - 1, TEAM, half, 128), jnp.float32),
                pltpu.VMEM((turns, TEAM, half, 128), jnp.float32),
                pltpu.VMEM((turns, half, 128), jnp.float32),
                dma((3, blk_n // 2)),
                dma((blk_n,)), dma((blk_n,)),
                dma, dma, dma, dma,
                dma((PIECES,)), dma,
                dma((PIECES,)), dma,
                dma((STEPS - 1,)), dma((STEPS - 1,)),
                dma, dma((turns,)),
                dma, dma((turns,)),
                pltpu.SemaphoreType.REGULAR,
            ],
            compiler_params=pltpu.CompilerParams(collective_id=0, has_side_effects=True, vmem_limit_bytes=67043328),
        )(ratings, mask, user_init.T, item_init.T)
        return ut.T, vt.T

    return jax.shard_map(local_run, mesh=mesh, in_specs=(row_spec, row_spec, row_spec, item_spec), out_specs=(row_spec, item_spec), check_vma=False)
```

```python
import functools
import math

import jax
import jax.numpy as jnp
from jax import lax
from jax.experimental import pallas as pl
from jax.experimental.pallas import tpu as pltpu
from jax.sharding import PartitionSpec as P

STEPS = 4
EPOCHS = 2
STEP_GAIN = 0.4
DECAY = 0.002
GROUPS = 4
TEAM = 4
PIECES = 4
MESH = pl.DeviceIdType.MESH


def kernel(dims, r_hbm, m_hbm, u_hbm, v_hbm, ut_out, vt_out, rbuf, mbuf, ubuf, vbuf, packed, work, usrc, uret, vown, vret, ut, uh, uth, wt, err, vst,
           xsend, slots, xslots, vslots, load_sem, ship_send, ship_recv, user_send, user_recv, item_send, item_recv, back_send, back_recv,
           final_send, final_recv, send_sem, recv_sem, xsend_sem, xrecv_sem, vsend_sem, vrecv_sem, credit):
    blk_n, step_size, decay_coef = dims
    rank, users = ubuf.shape
    rows = users // GROUPS
    half = rank // 2
    pairs = blk_n // 2
    me_b = lax.axis_index("blk")
    me_s = lax.axis_index("sub")
    x, core = me_b // 2, me_b % 2
    z, y = me_s // 4, me_s % 4

    out_y = (y // 2 + core + x) % 2
    out_z = z // 2
    piece = 2 * out_y + out_z
    target = {"sub": (z + out_z * (3 - 2 * z)) * 4 + y + out_y * (3 - 2 * y), "blk": 2 * x + 1}
    is_own = jnp.logical_and(core == 1, piece == 0)
    ships = jnp.logical_not(is_own)
    is_worker = jnp.logical_and(core == 1, z < 2)
    job_core = (y // 2 + x) % 2
    job = 2 * x + job_core
    has_own = job_core == 1
    place = (z % 2) * 2 + y % 2

    def source(q):
        oy, oz = q // 2, q % 2
        return {"sub": (z + oz * (3 - 2 * z)) * 4 + y + oy * (3 - 2 * y), "blk": job}

    def worker(block, p):
        bx = block // 2
        return {"sub": (p // 2) * 4 + 2 * ((block % 2 + bx) % 2) + p % 2, "blk": 2 * bx + 1}

    prev_job = (job + blk_n - 1) % blk_n
    next_job = (job + 1) % blk_n

    def mate(d, flip=0):
        dz, dy = d // 2, d % 2
        pz, py = (place // 2 + dz) % 2, (place % 2 + dy + flip) % 2
        return pz * 2 + py

    def load(q, src, dst, kind):
        col = pl.multiple_of(((x + q) % pairs) * 128, 128)
        return pltpu.make_async_copy(src.at[:, pl.ds(col, 128)], dst.at[q], load_sem.at[kind, q])

    load_users = pltpu.make_async_copy(u_hbm, ubuf, load_sem.at[2, 0])
    load_items = pltpu.make_async_copy(v_hbm, vbuf, load_sem.at[2, 1])
    load_users.start()
    load_items.start()
    load(0, r_hbm, rbuf, 0).start()
    load(0, m_hbm, mbuf, 1).start()

    barrier = pltpu.get_barrier_semaphore()

    def greet(device):
        pl.semaphore_signal(barrier, inc=1, device_id=device, device_id_type=MESH)

    @pl.when(ships)
    def _():
        greet(target)

    @pl.when(is_worker)
    def _():
        for q in range(1, PIECES):
            greet(source(q))

        @pl.when(jnp.logical_not(has_own))
        def _():
            greet(source(0))

        for d in (3, 2, 1):
            greet(worker(job, mate(d)))
        for p in range(TEAM):
            greet(worker(prev_job, p))
            greet(worker(next_job, p))

    low = lax.broadcasted_iota(jnp.int32, (half, 128), 1) < 64
    left = lax.broadcasted_iota(jnp.int32, (rank, 128), 1) < 64

    load_users.wait()
    for g in range(GROUPS):
        usrc[g * rank:(g + 1) * rank, :] = ubuf[:, g * rows:(g + 1) * rows]
    load_items.wait()
    vown[:, 0:64] = vbuf[0:half, :]
    vown[:, 64:128] = vbuf[half:rank, :]

    @pl.when(jnp.logical_not(is_worker))
    def _():
        pl.semaphore_wait(barrier, 1)

    @pl.when(jnp.logical_and(is_worker, has_own))
    def _():
        pl.semaphore_wait(barrier, PIECES - 1 + TEAM - 1 + 2 * TEAM)

    @pl.when(jnp.logical_and(is_worker, jnp.logical_not(has_own)))
    def _():
        pl.semaphore_wait(barrier, PIECES + 1 + TEAM - 1 + 2 * TEAM)

    send_users = pltpu.make_async_remote_copy(
        src_ref=usrc, dst_ref=ut.at[piece], send_sem=user_send, recv_sem=user_recv, device_id=target, device_id_type=MESH)
    send_items = pltpu.make_async_remote_copy(
        src_ref=vown, dst_ref=vst, send_sem=item_send, recv_sem=item_recv, device_id=target, device_id_type=MESH)
    gives_items = jnp.logical_and(core == 0, piece == 0)

    @pl.when(ships)
    def _():
        send_users.start()

    @pl.when(gives_items)
    def _():
        send_items.start()

    def ship(k):
        column = (me_b + k) % blk_n
        return pltpu.make_async_remote_copy(
            src_ref=packed.at[column], dst_ref=work.at[column, piece], send_sem=ship_send.at[k], recv_sem=ship_recv.at[column],
            device_id=target, device_id_type=MESH)

    chunk = 64
    low_c = lax.broadcasted_iota(jnp.int32, (chunk, 128), 1) < 64

    def pack_pair(q):
        even = ((x + q) % pairs) * 2

        def pack_rows(c, carry):
            base = pl.multiple_of(c * chunk, chunk)
            for col in range(2):
                vals = []
                for g in (2 * col, 2 * col + 1):
                    src = pl.ds(g * rows + base, chunk)
                    vals.append(jnp.where(mbuf[q, src, :] != 0, rbuf[q, src, :], jnp.nan))
                x0, x1 = vals
                packed[even, pl.ds(base, chunk), col * 128:(col + 1) * 128] = jnp.where(low_c, x0, pltpu.roll(x1, 64, 1))
                packed[even + 1, pl.ds(base, chunk), col * 128:(col + 1) * 128] = jnp.where(low_c, pltpu.roll(x0, 64, 1), x1)
            return carry

        lax.fori_loop(0, rows // chunk, pack_rows, 0)

    load(0, r_hbm, rbuf, 0).wait()
    load(0, m_hbm, mbuf, 1).wait()
    for q in range(1, pairs):
        load(q, r_hbm, rbuf, 0).start()
        load(q, m_hbm, mbuf, 1).start()
    pack_pair(0)

    @pl.when(ships)
    def _():
        ship(0).start()

    def pack_rest(q, carry):
        load(q, r_hbm, rbuf, 0).wait()
        load(q, m_hbm, mbuf, 1).wait()
        pack_pair(q)
        return carry

    lax.fori_loop(1, pairs, pack_rest, 0)

    is_far = piece == 3

    @pl.when(is_far)
    def _():
        def ship_far(k, carry):
            pl.semaphore_wait(credit, 1)
            ship(k).start()
            ship(k - 1).wait_send()
            return carry

        lax.fori_loop(1, blk_n, ship_far, 0)
        ship(blk_n - 1).wait_send()

    @pl.when(jnp.logical_and(ships, jnp.logical_not(is_far)))
    def _():
        ship(1).start()

    @pl.when(jnp.logical_and(ships, jnp.logical_not(jnp.logical_or(is_worker, is_far))))
    def _():
        def ship_next(k, carry):
            ship(k - 2).wait_send()
            ship(k).start()
            return carry

        lax.fori_loop(2, blk_n, ship_next, 0)
        ship(blk_n - 2).wait_send()
        ship(blk_n - 1).wait_send()

    @pl.when(is_own)
    def _():
        def keep(column, carry):
            work[column, 0] = packed[column]
            return carry

        lax.fori_loop(0, blk_n, keep, 0)
        ut[0] = usrc[...]
        vst[...] = vown[...]

    def halves(q):
        new_half = ut[q].astype(jnp.bfloat16)
        uth[:, q * rows:(q + 1) * rows] = new_half
        uh[q * rows:(q + 1) * rows, :] = new_half.T

    def spread(vp):
        swapped = pltpu.roll(vp, 64, 1)
        full = jnp.concatenate([jnp.where(low, vp, swapped), jnp.where(low, swapped, vp)], axis=0)
        lo = jnp.where(left, full, 0.0).astype(jnp.bfloat16)
        hi = jnp.where(left, 0.0, full).astype(jnp.bfloat16)
        wt[0:rank, 0:128] = lo
        wt[rank:2 * rank, 0:128] = hi
        wt[2 * rank:3 * rank, 128:256] = lo
        wt[3 * rank:4 * rank, 128:256] = hi

    def partial(block):
        for q in range(PIECES):
            sl = slice(q * rows, (q + 1) * rows)
            predicted = jnp.dot(uh[sl, :], wt[...], preferred_element_type=jnp.float32)
            rate = work[block, q]
            err[sl, :] = jnp.where(rate == rate, predicted - rate, 0.0).astype(jnp.bfloat16)
        both = None
        for q in range(PIECES):
            sl = slice(q * rows, (q + 1) * rows)
            s = jnp.dot(uth[:, sl], err[sl, :], preferred_element_type=jnp.float32)
            s_lo = s[0:rank, 0:128] + s[2 * rank:3 * rank, 128:256]
            s_hi = s[rank:2 * rank, 0:128] + s[3 * rank:4 * rank, 128:256]
            part = jnp.where(left, s_lo, s_hi)
            both = part if both is None else both + part
        top, bottom = both[0:half], both[half:rank]
        return jnp.where(low, top, bottom) + pltpu.roll(jnp.where(low, bottom, top), 64, 1)

    def user_step():
        for q in range(PIECES):
            grad = lax.dot_general(wt[...], err[q * rows:(q + 1) * rows, :], (((1,), (1,)), ((), ())), preferred_element_type=jnp.float32)
            old = ut[q]
            ut[q] = old - step_size * (grad + decay_coef * old)
            halves(q)

    def item_step(parts):
        total = (parts[0] + parts[1]) + (parts[2] + parts[3])
        old = vst[...]
        return old - step_size * (total + decay_coef * old)

    def await_pieces(buf, sem):
        @pl.when(has_own)
        def _():
            most = buf.at[pl.ds(1, PIECES - 1)]
            pltpu.make_async_copy(most, most, sem).wait()

        @pl.when(jnp.logical_not(has_own))
        def _():
            pltpu.make_async_copy(buf, buf, sem).wait()

    def give_users(q):
        return pltpu.make_async_remote_copy(
            src_ref=ut.at[q], dst_ref=uret, send_sem=back_send.at[q], recv_sem=back_recv, device_id=source(q), device_id_type=MESH)

    def give_items(q):
        return pltpu.make_async_remote_copy(
            src_ref=vst, dst_ref=vret, send_sem=final_send.at[q], recv_sem=final_recv, device_id=source(q), device_id_type=MESH)

    def sub_epoch(t, carry):
        block = (job + t) % blk_n

        @pl.when(t < blk_n)
        def _():
            await_pieces(work.at[block], ship_recv.at[block])

        @pl.when(t < blk_n - 1)
        def _():
            pl.semaphore_signal(credit, inc=1, device_id=source(3), device_id_type=MESH)

        @pl.when(jnp.logical_and(ships, t < blk_n - 2))
        def _():
            ship(t).wait_send()
            ship(t + 2).start()

        for step in range(STEPS - 1):
            spread(vst[...])
            slots[step, place] = partial(block)
            for d in (3, 2, 1):
                pltpu.make_async_remote_copy(
                    src_ref=slots.at[step, place], dst_ref=slots.at[step, place], send_sem=send_sem.at[step], recv_sem=recv_sem.at[step],
                    device_id=worker(job, mate(d)), device_id_type=MESH).start()
            user_step()
            others = slots.at[step, pl.ds(0, TEAM - 1)]
            pltpu.make_async_copy(others, others, send_sem.at[step]).wait()
            pltpu.make_async_copy(others, others, recv_sem.at[step]).wait()
            vst[...] = item_step(slots[step])
        ahead = pltpu.make_async_remote_copy(
            src_ref=vst, dst_ref=vslots.at[t], send_sem=vsend_sem, recv_sem=vrecv_sem.at[t],
            device_id=worker(prev_job, place), device_id_type=MESH)
        ahead.start()
        spread(vst[...])
        xsend[...] = partial(block)
        for d in (3, 2, 1, 0):
            pltpu.make_async_remote_copy(
                src_ref=xsend, dst_ref=xslots.at[t, place], send_sem=xsend_sem, recv_sem=xrecv_sem.at[t],
                device_id=worker(prev_job, mate(d, job_core)), device_id_type=MESH).start()
        user_step()

        @pl.when(t == EPOCHS * blk_n - 1)
        def _():
            for q in (3, 1, 2):
                give_users(q).start()

            @pl.when(jnp.logical_not(has_own))
            def _():
                give_users(0).start()

        everyone = xslots.at[t]
        pltpu.make_async_copy(everyone, everyone, xsend_sem).wait()
        ahead.wait()
        pltpu.make_async_copy(everyone, everyone, xrecv_sem.at[t]).wait()
        vst[...] = vslots[t]
        vst[...] = item_step(xslots[t])
        return carry

    @pl.when(is_worker)
    def _():
        wt[...] = jnp.zeros_like(wt)
        await_pieces(ut, user_recv)

        @pl.when(jnp.logical_not(has_own))
        def _():
            pltpu.make_async_copy(vst, vst, item_recv).wait()

        for q in range(PIECES):
            halves(q)
        lax.fori_loop(0, EPOCHS * blk_n, sub_epoch, 0)
        for q in (3, 2, 1):
            give_items(q).start()

        @pl.when(jnp.logical_not(has_own))
        def _():
            give_items(0).start()

        @pl.when(ships)
        def _():
            ship(blk_n - 2).wait_send()
            ship(blk_n - 1).wait_send()

    @pl.when(ships)
    def _():
        send_users.wait_send()
        pltpu.make_async_copy(uret, uret, back_recv).wait()
        pltpu.make_async_copy(vret, vret, final_recv).wait()
        for g in range(GROUPS):
            ut_out[:, g * rows:(g + 1) * rows] = uret[g * rank:(g + 1) * rank, :]
        vt_out[0:half, :] = vret[:, 0:64]
        vt_out[half:rank, :] = vret[:, 64:128]

    @pl.when(gives_items)
    def _():
        send_items.wait_send()

    @pl.when(is_own)
    def _():
        for g in range(GROUPS):
            ut_out[:, g * rows:(g + 1) * rows] = ut[0, g * rank:(g + 1) * rank, :]
        vt_out[0:half, :] = vst[:, 0:64]
        vt_out[half:rank, :] = vst[:, 64:128]

    @pl.when(is_worker)
    def _():
        for q in (3, 2, 1):
            give_users(q).wait_send()
            give_items(q).wait_send()

        @pl.when(jnp.logical_not(has_own))
        def _():
            give_users(0).wait_send()
            give_items(0).wait_send()


def solution(mesh):
    blk_n = mesh.shape["blk"]
    sub_n = mesh.shape["sub"]
    row_spec = P(("rep", "blk", "sub"), None)
    item_spec = P(("rep", "blk"), None)

    def local_run(ratings, mask, user_init, item_init):
        users = ratings.shape[0]
        items, rank = item_init.shape
        big_side = max(items, sub_n * users)
        step_size = STEP_GAIN * math.sqrt(rank) / (math.sqrt(big_side) + math.sqrt(rank)) ** 2
        decay_coef = DECAY / step_size
        rows = users // GROUPS
        turns = EPOCHS * blk_n
        half = rank // 2
        wide_u, wide_i = GROUPS * rank, GROUPS * items
        vmem = pl.BlockSpec(memory_space=pltpu.VMEM)
        dma = pltpu.SemaphoreType.DMA
        ut, vt = pl.pallas_call(
            functools.partial(kernel, (blk_n, step_size, decay_coef)),
            out_shape=(jax.ShapeDtypeStruct((rank, users), jnp.float32), jax.ShapeDtypeStruct((rank, items), jnp.float32)),
            in_specs=[pl.BlockSpec(memory_space=pl.ANY)] * 4,
            out_specs=(vmem, vmem),
            scratch_shapes=[
                pltpu.VMEM((blk_n // 2, users, 128), jnp.float32),
                pltpu.VMEM((blk_n // 2, users, 128), jnp.int32),
                pltpu.VMEM((rank, users), jnp.float32),
                pltpu.VMEM((rank, items), jnp.float32),
                pltpu.VMEM((blk_n, rows, wide_i), jnp.float32),
                pltpu.VMEM((blk_n, PIECES, rows, wide_i), jnp.float32),
                pltpu.VMEM((wide_u, rows), jnp.float32),
                pltpu.VMEM((wide_u, rows), jnp.float32),
                pltpu.VMEM((half, 128), jnp.float32),
                pltpu.VMEM((half, 128), jnp.float32),
                pltpu.VMEM((PIECES, wide_u, rows), jnp.float32),
                pltpu.VMEM((PIECES * rows, wide_u), jnp.bfloat16),
                pltpu.VMEM((wide_u, PIECES * rows), jnp.bfloat16),
                pltpu.VMEM((wide_u, wide_i), jnp.bfloat16),
                pltpu.VMEM((PIECES * rows, wide_i), jnp.bfloat16),
                pltpu.VMEM((half, 128), jnp.float32),
                pltpu.VMEM((half, 128), jnp.float32),
                pltpu.VMEM((STEPS - 1, TEAM, half, 128), jnp.float32),
                pltpu.VMEM((turns, TEAM, half, 128), jnp.float32),
                pltpu.VMEM((turns, half, 128), jnp.float32),
                dma((3, blk_n // 2)),
                dma((blk_n,)), dma((blk_n,)),
                dma, dma, dma, dma,
                dma((PIECES,)), dma,
                dma((PIECES,)), dma,
                dma((STEPS - 1,)), dma((STEPS - 1,)),
                dma, dma((turns,)),
                dma, dma((turns,)),
                pltpu.SemaphoreType.REGULAR,
            ],
            compiler_params=pltpu.CompilerParams(collective_id=0, has_side_effects=True, vmem_limit_bytes=53 * 1024 * 1024),
        )(ratings, mask, user_init.T, item_init.T)
        return ut.T, vt.T

    return jax.shard_map(local_run, mesh=mesh, in_specs=(row_spec, row_spec, row_spec, item_spec), out_specs=(row_spec, item_spec), check_vma=False)
```

```python
import functools
import math

import jax
import jax.numpy as jnp
from jax import lax
from jax.experimental import pallas as pl
from jax.experimental.pallas import tpu as pltpu
from jax.sharding import PartitionSpec as P

STEPS = 4
EPOCHS = 2
STEP_GAIN = 0.4
DECAY = 0.002
GROUPS = 4
TEAM = 4
PIECES = 4
SPLIT = (3, 3, 1, 1)
MESH = pl.DeviceIdType.MESH


def kernel(dims, r_hbm, m_hbm, ubuf, vbuf, ut_out, vt_out, rbuf, mbuf, packed, work, usrc, uret, vown, vret, ut, uh, uth, wt, err, vst,
           xsend, slots, xslots, vslots, load_sem, ship_send, ship_recv, user_send, user_recv, item_send, item_recv, back_send, back_recv,
           final_send, final_recv, send_sem, recv_sem, xsend_sem, xrecv_sem, vsend_sem, vrecv_sem, credit):
    blk_n, step_size, decay_coef = dims
    rank, users = ubuf.shape
    rows = users // GROUPS
    half = rank // 2
    pairs = blk_n // 2
    me_b = lax.axis_index("blk")
    me_s = lax.axis_index("sub")
    x, core = me_b // 2, me_b % 2
    z, y = me_s // 4, me_s % 4

    out_y = (y // 2 + core + x) % 2
    out_z = z // 2
    piece = 2 * out_y + out_z
    target = {"sub": (z + out_z * (3 - 2 * z)) * 4 + y + out_y * (3 - 2 * y), "blk": 2 * x + 1}
    is_own = jnp.logical_and(core == 1, piece == 0)
    ships = jnp.logical_not(is_own)
    is_worker = jnp.logical_and(core == 1, z < 2)
    job_core = (y // 2 + x) % 2
    job = 2 * x + job_core
    has_own = job_core == 1
    place = (z % 2) * 2 + y % 2

    def source(q):
        oy, oz = q // 2, q % 2
        return {"sub": (z + oz * (3 - 2 * z)) * 4 + y + oy * (3 - 2 * y), "blk": job}

    def worker(block, p):
        bx = block // 2
        return {"sub": (p // 2) * 4 + 2 * ((block % 2 + bx) % 2) + p % 2, "blk": 2 * bx + 1}

    prev_job = (job + blk_n - 1) % blk_n
    next_job = (job + 1) % blk_n

    def mate(d, flip=0):
        dz, dy = d // 2, d % 2
        pz, py = (place // 2 + dz) % 2, (place % 2 + dy + flip) % 2
        return pz * 2 + py

    def load(q, src, dst, kind):
        col = pl.multiple_of(((x + q) % pairs) * 128, 128)
        return pltpu.make_async_copy(src.at[:, pl.ds(col, 128)], dst.at[q], load_sem.at[kind, q])

    load(0, r_hbm, rbuf, 0).start()
    load(0, m_hbm, mbuf, 1).start()

    barrier = pltpu.get_barrier_semaphore()

    def greet(device):
        pl.semaphore_signal(barrier, inc=1, device_id=device, device_id_type=MESH)

    @pl.when(ships)
    def _():
        greet(target)

    @pl.when(is_worker)
    def _():
        for q in range(1, PIECES):
            greet(source(q))

        @pl.when(jnp.logical_not(has_own))
        def _():
            greet(source(0))

        for d in (3, 2, 1):
            greet(worker(job, mate(d)))
        for p in range(TEAM):
            greet(worker(prev_job, p))
            greet(worker(next_job, p))

    low = lax.broadcasted_iota(jnp.int32, (half, 128), 1) < 64
    left = lax.broadcasted_iota(jnp.int32, (rank, 128), 1) < 64

    for g in range(GROUPS):
        usrc[g * rank:(g + 1) * rank, :] = ubuf[:, g * rows:(g + 1) * rows]
    vown[:, 0:64] = vbuf[0:half, :]
    vown[:, 64:128] = vbuf[half:rank, :]

    @pl.when(jnp.logical_not(is_worker))
    def _():
        pl.semaphore_wait(barrier, 1)

    @pl.when(jnp.logical_and(is_worker, has_own))
    def _():
        pl.semaphore_wait(barrier, PIECES - 1 + TEAM - 1 + 2 * TEAM)

    @pl.when(jnp.logical_and(is_worker, jnp.logical_not(has_own)))
    def _():
        pl.semaphore_wait(barrier, PIECES + 1 + TEAM - 1 + 2 * TEAM)

    send_users = pltpu.make_async_remote_copy(
        src_ref=usrc, dst_ref=ut.at[piece], send_sem=user_send, recv_sem=user_recv, device_id=target, device_id_type=MESH)
    send_items = pltpu.make_async_remote_copy(
        src_ref=vown, dst_ref=vst, send_sem=item_send, recv_sem=item_recv, device_id=target, device_id_type=MESH)
    gives_items = jnp.logical_and(core == 0, piece == 0)

    @pl.when(ships)
    def _():
        send_users.start()

    @pl.when(gives_items)
    def _():
        send_items.start()

    def ship(k):
        column = (me_b + k) % blk_n
        return pltpu.make_async_remote_copy(
            src_ref=packed.at[column], dst_ref=work.at[column, piece], send_sem=ship_send.at[k], recv_sem=ship_recv.at[column],
            device_id=target, device_id_type=MESH)

    chunk = 64
    low_c = lax.broadcasted_iota(jnp.int32, (chunk, 128), 1) < 64

    def pack_pair(q):
        even = ((x + q) % pairs) * 2

        def pack_rows(c, carry):
            base = pl.multiple_of(c * chunk, chunk)
            for col in range(2):
                vals = []
                for g in (2 * col, 2 * col + 1):
                    src = pl.ds(g * rows + base, chunk)
                    vals.append(jnp.where(mbuf[q, src, :] != 0, rbuf[q, src, :], jnp.nan))
                x0, x1 = vals
                packed[even, pl.ds(base, chunk), col * 128:(col + 1) * 128] = jnp.where(low_c, x0, pltpu.roll(x1, 64, 1))
                packed[even + 1, pl.ds(base, chunk), col * 128:(col + 1) * 128] = jnp.where(low_c, pltpu.roll(x0, 64, 1), x1)
            return carry

        lax.fori_loop(0, rows // chunk, pack_rows, 0)

    load(0, r_hbm, rbuf, 0).wait()
    load(0, m_hbm, mbuf, 1).wait()
    for q in range(1, pairs):
        load(q, r_hbm, rbuf, 0).start()
        load(q, m_hbm, mbuf, 1).start()
    pack_pair(0)

    @pl.when(ships)
    def _():
        ship(0).start()

    def pack_rest(q, carry):
        load(q, r_hbm, rbuf, 0).wait()
        load(q, m_hbm, mbuf, 1).wait()
        pack_pair(q)
        return carry

    lax.fori_loop(1, pairs, pack_rest, 0)

    is_far = piece == 3

    @pl.when(is_far)
    def _():
        def ship_far(k, carry):
            pl.semaphore_wait(credit, 1)
            ship(k).start()
            ship(k - 1).wait_send()
            return carry

        lax.fori_loop(1, blk_n, ship_far, 0)
        ship(blk_n - 1).wait_send()

    @pl.when(jnp.logical_and(ships, jnp.logical_not(is_far)))
    def _():
        ship(1).start()

    @pl.when(jnp.logical_and(ships, jnp.logical_not(jnp.logical_or(is_worker, is_far))))
    def _():
        def ship_next(k, carry):
            ship(k - 2).wait_send()
            ship(k).start()
            return carry

        lax.fori_loop(2, blk_n, ship_next, 0)
        ship(blk_n - 2).wait_send()
        ship(blk_n - 1).wait_send()

    @pl.when(is_own)
    def _():
        def keep(column, carry):
            work[column, 0] = packed[column]
            return carry

        lax.fori_loop(0, blk_n, keep, 0)
        ut[0] = usrc[...]
        vst[...] = vown[...]

    def halves(q):
        new_half = ut[q].astype(jnp.bfloat16)
        uth[:, q * rows:(q + 1) * rows] = new_half
        uh[q * rows:(q + 1) * rows, :] = new_half.T

    def spread(vp):
        swapped = pltpu.roll(vp, 64, 1)
        full = jnp.concatenate([jnp.where(low, vp, swapped), jnp.where(low, swapped, vp)], axis=0)
        lo = jnp.where(left, full, 0.0).astype(jnp.bfloat16)
        hi = jnp.where(left, 0.0, full).astype(jnp.bfloat16)
        wt[0:rank, 0:128] = lo
        wt[rank:2 * rank, 0:128] = hi
        wt[2 * rank:3 * rank, 128:256] = lo
        wt[3 * rank:4 * rank, 128:256] = hi

    def partial(block):
        for q in range(PIECES):
            sl = slice(q * rows, (q + 1) * rows)
            predicted = jnp.dot(uh[sl, :], wt[...], preferred_element_type=jnp.float32)
            rate = work[block, q]
            err[sl, :] = jnp.where(rate == rate, predicted - rate, 0.0).astype(jnp.bfloat16)
        both = None
        start = 0
        for share in SPLIT:
            sl = slice(start, start + share * PIECES * rows // sum(SPLIT))
            start = sl.stop
            s = jnp.dot(uth[:, sl], err[sl, :], preferred_element_type=jnp.float32)
            s_lo = s[0:rank, 0:128] + s[2 * rank:3 * rank, 128:256]
            s_hi = s[rank:2 * rank, 0:128] + s[3 * rank:4 * rank, 128:256]
            part = jnp.where(left, s_lo, s_hi)
            both = part if both is None else both + part
        top, bottom = both[0:half], both[half:rank]
        return jnp.where(low, top, bottom) + pltpu.roll(jnp.where(low, bottom, top), 64, 1)

    def user_step():
        for q in range(PIECES):
            grad = lax.dot_general(wt[...], err[q * rows:(q + 1) * rows, :], (((1,), (1,)), ((), ())), preferred_element_type=jnp.float32)
            old = ut[q]
            ut[q] = old - step_size * (grad + decay_coef * old)
            halves(q)

    def item_step(old, parts):
        total = (parts[0] + parts[1]) + (parts[2] + parts[3])
        return old - step_size * (total + decay_coef * old)

    def await_pieces(buf, sem):
        @pl.when(has_own)
        def _():
            most = buf.at[pl.ds(1, PIECES - 1)]
            pltpu.make_async_copy(most, most, sem).wait()

        @pl.when(jnp.logical_not(has_own))
        def _():
            pltpu.make_async_copy(buf, buf, sem).wait()

    def give_users(q):
        return pltpu.make_async_remote_copy(
            src_ref=ut.at[q], dst_ref=uret, send_sem=back_send.at[q], recv_sem=back_recv, device_id=source(q), device_id_type=MESH)

    def give_items(q):
        return pltpu.make_async_remote_copy(
            src_ref=vst, dst_ref=vret, send_sem=final_send.at[q], recv_sem=final_recv, device_id=source(q), device_id_type=MESH)

    def sub_epoch(t, vp):
        block = (job + t) % blk_n

        @pl.when(t < blk_n)
        def _():
            await_pieces(work.at[block], ship_recv.at[block])

        @pl.when(t < blk_n - 1)
        def _():
            pl.semaphore_signal(credit, inc=1, device_id=source(3), device_id_type=MESH)

        @pl.when(jnp.logical_and(ships, t < blk_n - 2))
        def _():
            ship(t).wait_send()
            ship(t + 2).start()

        for step in range(STEPS - 1):
            spread(vp)
            slots[step, place] = partial(block)
            for d in (3, 2, 1):
                pltpu.make_async_remote_copy(
                    src_ref=slots.at[step, place], dst_ref=slots.at[step, place], send_sem=send_sem.at[step], recv_sem=recv_sem.at[step],
                    device_id=worker(job, mate(d)), device_id_type=MESH).start()
            user_step()
            others = slots.at[step, pl.ds(0, TEAM - 1)]
            pltpu.make_async_copy(others, others, send_sem.at[step]).wait()
            pltpu.make_async_copy(others, others, recv_sem.at[step]).wait()
            vp = item_step(vp, slots[step])
        vst[...] = vp
        ahead = pltpu.make_async_remote_copy(
            src_ref=vst, dst_ref=vslots.at[t], send_sem=vsend_sem, recv_sem=vrecv_sem.at[t],
            device_id=worker(prev_job, place), device_id_type=MESH)
        ahead.start()
        spread(vp)
        xsend[...] = partial(block)
        for d in (3, 2, 1, 0):
            pltpu.make_async_remote_copy(
                src_ref=xsend, dst_ref=xslots.at[t, place], send_sem=xsend_sem, recv_sem=xrecv_sem.at[t],
                device_id=worker(prev_job, mate(d, job_core)), device_id_type=MESH).start()
        user_step()

        @pl.when(t == EPOCHS * blk_n - 1)
        def _():
            for q in (3, 1, 2):
                give_users(q).start()

            @pl.when(jnp.logical_not(has_own))
            def _():
                give_users(0).start()

        everyone = xslots.at[t]
        pltpu.make_async_copy(everyone, everyone, xsend_sem).wait()
        ahead.wait()
        pltpu.make_async_copy(everyone, everyone, xrecv_sem.at[t]).wait()
        return item_step(vslots[t], xslots[t])

    @pl.when(is_worker)
    def _():
        wt[...] = jnp.zeros_like(wt)
        await_pieces(ut, user_recv)

        @pl.when(jnp.logical_not(has_own))
        def _():
            pltpu.make_async_copy(vst, vst, item_recv).wait()

        for q in range(PIECES):
            halves(q)
        vst[...] = lax.fori_loop(0, EPOCHS * blk_n, sub_epoch, vst[...])
        for q in (3, 2, 1):
            give_items(q).start()

        @pl.when(jnp.logical_not(has_own))
        def _():
            give_items(0).start()

        @pl.when(ships)
        def _():
            ship(blk_n - 2).wait_send()
            ship(blk_n - 1).wait_send()

    @pl.when(ships)
    def _():
        send_users.wait_send()
        pltpu.make_async_copy(uret, uret, back_recv).wait()
        pltpu.make_async_copy(vret, vret, final_recv).wait()
        for g in range(GROUPS):
            ut_out[:, g * rows:(g + 1) * rows] = uret[g * rank:(g + 1) * rank, :]
        vt_out[0:half, :] = vret[:, 0:64]
        vt_out[half:rank, :] = vret[:, 64:128]

    @pl.when(gives_items)
    def _():
        send_items.wait_send()

    @pl.when(is_own)
    def _():
        for g in range(GROUPS):
            ut_out[:, g * rows:(g + 1) * rows] = ut[0, g * rank:(g + 1) * rank, :]
        vt_out[0:half, :] = vst[:, 0:64]
        vt_out[half:rank, :] = vst[:, 64:128]

    @pl.when(is_worker)
    def _():
        for q in (3, 2, 1):
            give_users(q).wait_send()
            give_items(q).wait_send()

        @pl.when(jnp.logical_not(has_own))
        def _():
            give_users(0).wait_send()
            give_items(0).wait_send()


def solution(mesh):
    blk_n = mesh.shape["blk"]
    sub_n = mesh.shape["sub"]
    row_spec = P(("rep", "blk", "sub"), None)
    item_spec = P(("rep", "blk"), None)

    def local_run(ratings, mask, user_init, item_init):
        users = ratings.shape[0]
        items, rank = item_init.shape
        big_side = max(items, sub_n * users)
        step_size = STEP_GAIN * math.sqrt(rank) / (math.sqrt(big_side) + math.sqrt(rank)) ** 2
        decay_coef = DECAY / step_size
        rows = users // GROUPS
        turns = EPOCHS * blk_n
        half = rank // 2
        wide_u, wide_i = GROUPS * rank, GROUPS * items
        vmem = pl.BlockSpec(memory_space=pltpu.VMEM)
        dma = pltpu.SemaphoreType.DMA
        ut, vt = pl.pallas_call(
            functools.partial(kernel, (blk_n, step_size, decay_coef)),
            out_shape=(jax.ShapeDtypeStruct((rank, users), jnp.float32), jax.ShapeDtypeStruct((rank, items), jnp.float32)),
            in_specs=[pl.BlockSpec(memory_space=pl.ANY)] * 2 + [vmem] * 2,
            out_specs=(vmem, vmem),
            scratch_shapes=[
                pltpu.VMEM((blk_n // 2, users, 128), jnp.float32),
                pltpu.VMEM((blk_n // 2, users, 128), jnp.int32),
                pltpu.VMEM((blk_n, rows, wide_i), jnp.float32),
                pltpu.VMEM((blk_n, PIECES, rows, wide_i), jnp.float32),
                pltpu.VMEM((wide_u, rows), jnp.float32),
                pltpu.VMEM((wide_u, rows), jnp.float32),
                pltpu.VMEM((half, 128), jnp.float32),
                pltpu.VMEM((half, 128), jnp.float32),
                pltpu.VMEM((PIECES, wide_u, rows), jnp.float32),
                pltpu.VMEM((PIECES * rows, wide_u), jnp.bfloat16),
                pltpu.VMEM((wide_u, PIECES * rows), jnp.bfloat16),
                pltpu.VMEM((wide_u, wide_i), jnp.bfloat16),
                pltpu.VMEM((PIECES * rows, wide_i), jnp.bfloat16),
                pltpu.VMEM((half, 128), jnp.float32),
                pltpu.VMEM((half, 128), jnp.float32),
                pltpu.VMEM((STEPS - 1, TEAM, half, 128), jnp.float32),
                pltpu.VMEM((turns, TEAM, half, 128), jnp.float32),
                pltpu.VMEM((turns, half, 128), jnp.float32),
                dma((2, blk_n // 2)),
                dma((blk_n,)), dma((blk_n,)),
                dma, dma, dma, dma,
                dma((PIECES,)), dma,
                dma((PIECES,)), dma,
                dma((STEPS - 1,)), dma((STEPS - 1,)),
                dma, dma((turns,)),
                dma, dma((turns,)),
                pltpu.SemaphoreType.REGULAR,
            ],
            compiler_params=pltpu.CompilerParams(collective_id=0, has_side_effects=True, vmem_limit_bytes=53 * 1024 * 1024),
        )(ratings, mask, user_init.T, item_init.T)
        return ut.T, vt.T

    return jax.shard_map(local_run, mesh=mesh, in_specs=(row_spec, row_spec, row_spec, item_spec), out_specs=(row_spec, item_spec), check_vma=False)
```

```python
import functools
import math

import jax
import jax.numpy as jnp
from jax import lax
from jax.experimental import pallas as pl
from jax.experimental.pallas import tpu as pltpu
from jax.sharding import PartitionSpec as P

STEPS = 4
EPOCHS = 2
STEP_GAIN = 0.4
DECAY = 0.002
GROUPS = 4
TEAM = 4
PIECES = 4
SPLIT = (3, 3, 2)
MESH = pl.DeviceIdType.MESH


def kernel(dims, r_hbm, m_hbm, u_hbm, v_hbm, ut_out, vt_out, rbuf, mbuf, ubuf, vbuf, packed, work, usrc, uret, vown, vret, ut, uh, uth, wt, err, vst,
           xsend, slots, xslots, vslots, load_sem, ship_send, ship_recv, user_send, user_recv, item_send, item_recv, back_send, back_recv,
           final_send, final_recv, send_sem, recv_sem, xsend_sem, xrecv_sem, vsend_sem, vrecv_sem, credit):
    blk_n, step_size, decay_coef = dims
    rank, users = ubuf.shape
    rows = users // GROUPS
    half = rank // 2
    pairs = blk_n // 2
    me_b = lax.axis_index("blk")
    me_s = lax.axis_index("sub")
    x, core = me_b // 2, me_b % 2
    z, y = me_s // 4, me_s % 4

    out_y = (y // 2 + core + x) % 2
    out_z = z // 2
    piece = 2 * out_y + out_z
    target = {"sub": (z + out_z * (3 - 2 * z)) * 4 + y + out_y * (3 - 2 * y), "blk": 2 * x + 1}
    is_own = jnp.logical_and(core == 1, piece == 0)
    ships = jnp.logical_not(is_own)
    is_worker = jnp.logical_and(core == 1, z < 2)
    job_core = (y // 2 + x) % 2
    job = 2 * x + job_core
    has_own = job_core == 1
    place = (z % 2) * 2 + y % 2

    def source(q):
        oy, oz = q // 2, q % 2
        return {"sub": (z + oz * (3 - 2 * z)) * 4 + y + oy * (3 - 2 * y), "blk": job}

    def worker(block, p):
        bx = block // 2
        return {"sub": (p // 2) * 4 + 2 * ((block % 2 + bx) % 2) + p % 2, "blk": 2 * bx + 1}

    prev_job = (job + blk_n - 1) % blk_n
    next_job = (job + 1) % blk_n

    def mate(d, flip=0):
        dz, dy = d // 2, d % 2
        pz, py = (place // 2 + dz) % 2, (place % 2 + dy + flip) % 2
        return pz * 2 + py

    def load(q, src, dst, kind):
        col = pl.multiple_of(((x + q) % pairs) * 128, 128)
        return pltpu.make_async_copy(src.at[:, pl.ds(col, 128)], dst.at[q], load_sem.at[kind, q])

    load_users = pltpu.make_async_copy(u_hbm, ubuf, load_sem.at[2, 0])
    load_items = pltpu.make_async_copy(v_hbm, vbuf, load_sem.at[2, 1])
    load_users.start()
    load_items.start()
    load(0, r_hbm, rbuf, 0).start()
    load(0, m_hbm, mbuf, 1).start()

    barrier = pltpu.get_barrier_semaphore()

    def greet(device):
        pl.semaphore_signal(barrier, inc=1, device_id=device, device_id_type=MESH)

    @pl.when(ships)
    def _():
        greet(target)

    @pl.when(is_worker)
    def _():
        for q in range(1, PIECES):
            greet(source(q))

        @pl.when(jnp.logical_not(has_own))
        def _():
            greet(source(0))

        for d in (3, 2, 1):
            greet(worker(job, mate(d)))
        for p in range(TEAM):
            greet(worker(prev_job, p))
            greet(worker(next_job, p))

    low = lax.broadcasted_iota(jnp.int32, (half, 128), 1) < 64
    left = lax.broadcasted_iota(jnp.int32, (rank, 128), 1) < 64

    load_users.wait()
    for g in range(GROUPS):
        usrc[g * rank:(g + 1) * rank, :] = ubuf[:, g * rows:(g + 1) * rows]
    load_items.wait()
    vown[:, 0:64] = vbuf[0:half, :]
    vown[:, 64:128] = vbuf[half:rank, :]

    @pl.when(jnp.logical_not(is_worker))
    def _():
        pl.semaphore_wait(barrier, 1)

    @pl.when(jnp.logical_and(is_worker, has_own))
    def _():
        pl.semaphore_wait(barrier, PIECES - 1 + TEAM - 1 + 2 * TEAM)

    @pl.when(jnp.logical_and(is_worker, jnp.logical_not(has_own)))
    def _():
        pl.semaphore_wait(barrier, PIECES + 1 + TEAM - 1 + 2 * TEAM)

    send_users = pltpu.make_async_remote_copy(
        src_ref=usrc, dst_ref=ut.at[piece], send_sem=user_send, recv_sem=user_recv, device_id=target, device_id_type=MESH)
    send_items = pltpu.make_async_remote_copy(
        src_ref=vown, dst_ref=vst, send_sem=item_send, recv_sem=item_recv, device_id=target, device_id_type=MESH)
    gives_items = jnp.logical_and(core == 0, piece == 0)

    @pl.when(ships)
    def _():
        send_users.start()

    @pl.when(gives_items)
    def _():
        send_items.start()

    def ship(k):
        column = (me_b + k) % blk_n
        return pltpu.make_async_remote_copy(
            src_ref=packed.at[column], dst_ref=work.at[column, piece], send_sem=ship_send.at[k], recv_sem=ship_recv.at[column],
            device_id=target, device_id_type=MESH)

    chunk = 64
    low_c = lax.broadcasted_iota(jnp.int32, (chunk, 128), 1) < 64

    def pack_pair(q):
        even = ((x + q) % pairs) * 2

        def pack_rows(c, carry):
            base = pl.multiple_of(c * chunk, chunk)
            for col in range(2):
                vals = []
                for g in (2 * col, 2 * col + 1):
                    src = pl.ds(g * rows + base, chunk)
                    vals.append(jnp.where(mbuf[q, src, :] != 0, rbuf[q, src, :], jnp.nan))
                x0, x1 = vals
                packed[even, pl.ds(base, chunk), col * 128:(col + 1) * 128] = jnp.where(low_c, x0, pltpu.roll(x1, 64, 1))
                packed[even + 1, pl.ds(base, chunk), col * 128:(col + 1) * 128] = jnp.where(low_c, pltpu.roll(x0, 64, 1), x1)
            return carry

        lax.fori_loop(0, rows // chunk, pack_rows, 0)

    load(0, r_hbm, rbuf, 0).wait()
    load(0, m_hbm, mbuf, 1).wait()
    for q in range(1, pairs):
        load(q, r_hbm, rbuf, 0).start()
        load(q, m_hbm, mbuf, 1).start()
    pack_pair(0)

    @pl.when(ships)
    def _():
        ship(0).start()

    def pack_rest(q, carry):
        load(q, r_hbm, rbuf, 0).wait()
        load(q, m_hbm, mbuf, 1).wait()
        pack_pair(q)
        return carry

    lax.fori_loop(1, pairs, pack_rest, 0)

    is_far = piece == 3

    @pl.when(is_far)
    def _():
        def ship_far(k, carry):
            pl.semaphore_wait(credit, 1)
            ship(k).start()
            ship(k - 1).wait_send()
            return carry

        lax.fori_loop(1, blk_n, ship_far, 0)
        ship(blk_n - 1).wait_send()

    @pl.when(jnp.logical_and(ships, jnp.logical_not(is_far)))
    def _():
        ship(1).start()

    @pl.when(jnp.logical_and(ships, jnp.logical_not(jnp.logical_or(is_worker, is_far))))
    def _():
        def ship_next(k, carry):
            ship(k - 2).wait_send()
            ship(k).start()
            return carry

        lax.fori_loop(2, blk_n, ship_next, 0)
        ship(blk_n - 2).wait_send()
        ship(blk_n - 1).wait_send()

    @pl.when(is_own)
    def _():
        def keep(column, carry):
            work[column, 0] = packed[column]
            return carry

        lax.fori_loop(0, blk_n, keep, 0)
        ut[0] = usrc[...]
        vst[...] = vown[...]

    def halves(q):
        new_half = ut[q].astype(jnp.bfloat16)
        uth[:, q * rows:(q + 1) * rows] = new_half
        uh[q * rows:(q + 1) * rows, :] = new_half.T

    def spread(vp):
        swapped = pltpu.roll(vp, 64, 1)
        full = jnp.concatenate([jnp.where(low, vp, swapped), jnp.where(low, swapped, vp)], axis=0)
        lo = jnp.where(left, full, 0.0).astype(jnp.bfloat16)
        hi = jnp.where(left, 0.0, full).astype(jnp.bfloat16)
        wt[0:rank, 0:128] = lo
        wt[rank:2 * rank, 0:128] = hi
        wt[2 * rank:3 * rank, 128:256] = lo
        wt[3 * rank:4 * rank, 128:256] = hi

    def partial(block):
        for q in range(PIECES):
            sl = slice(q * rows, (q + 1) * rows)
            predicted = jnp.dot(uh[sl, :], wt[...], preferred_element_type=jnp.float32)
            rate = work[block, q]
            err[sl, :] = jnp.where(rate == rate, predicted - rate, 0.0).astype(jnp.bfloat16)
        both = None
        start = 0
        for share in SPLIT:
            sl = slice(start, start + share * PIECES * rows // sum(SPLIT))
            start = sl.stop
            s = jnp.dot(uth[:, sl], err[sl, :], preferred_element_type=jnp.float32)
            s_lo = s[0:rank, 0:128] + s[2 * rank:3 * rank, 128:256]
            s_hi = s[rank:2 * rank, 0:128] + s[3 * rank:4 * rank, 128:256]
            part = jnp.where(left, s_lo, s_hi)
            both = part if both is None else both + part
        top, bottom = both[0:half], both[half:rank]
        return jnp.where(low, top, bottom) + pltpu.roll(jnp.where(low, bottom, top), 64, 1)

    def user_step():
        for q in range(PIECES):
            grad = lax.dot_general(wt[...], err[q * rows:(q + 1) * rows, :], (((1,), (1,)), ((), ())), preferred_element_type=jnp.float32)
            old = ut[q]
            ut[q] = old - step_size * (grad + decay_coef * old)
            halves(q)

    def item_step(old, parts):
        total = (parts[0] + parts[1]) + (parts[2] + parts[3])
        return old - step_size * (total + decay_coef * old)

    def await_pieces(buf, sem):
        @pl.when(has_own)
        def _():
            most = buf.at[pl.ds(1, PIECES - 1)]
            pltpu.make_async_copy(most, most, sem).wait()

        @pl.when(jnp.logical_not(has_own))
        def _():
            pltpu.make_async_copy(buf, buf, sem).wait()

    def give_users(q):
        return pltpu.make_async_remote_copy(
            src_ref=ut.at[q], dst_ref=uret, send_sem=back_send.at[q], recv_sem=back_recv, device_id=source(q), device_id_type=MESH)

    def give_items(q):
        return pltpu.make_async_remote_copy(
            src_ref=vst, dst_ref=vret, send_sem=final_send.at[q], recv_sem=final_recv, device_id=source(q), device_id_type=MESH)

    def sub_epoch(t, vp):
        block = (job + t) % blk_n

        @pl.when(t < blk_n)
        def _():
            await_pieces(work.at[block], ship_recv.at[block])

        @pl.when(t < blk_n - 1)
        def _():
            pl.semaphore_signal(credit, inc=1, device_id=source(3), device_id_type=MESH)

        @pl.when(jnp.logical_and(ships, t < blk_n - 2))
        def _():
            ship(t).wait_send()
            ship(t + 2).start()

        for step in range(STEPS - 1):
            spread(vp)
            slots[step, place] = partial(block)
            for d in (3, 2, 1):
                pltpu.make_async_remote_copy(
                    src_ref=slots.at[step, place], dst_ref=slots.at[step, place], send_sem=send_sem.at[step], recv_sem=recv_sem.at[step],
                    device_id=worker(job, mate(d)), device_id_type=MESH).start()
            user_step()
            others = slots.at[step, pl.ds(0, TEAM - 1)]
            pltpu.make_async_copy(others, others, send_sem.at[step]).wait()
            pltpu.make_async_copy(others, others, recv_sem.at[step]).wait()
            vp = item_step(vp, slots[step])
        vst[...] = vp
        ahead = pltpu.make_async_remote_copy(
            src_ref=vst, dst_ref=vslots.at[t], send_sem=vsend_sem, recv_sem=vrecv_sem.at[t],
            device_id=worker(prev_job, place), device_id_type=MESH)
        ahead.start()
        spread(vp)
        xsend[...] = partial(block)
        for d in (3, 2, 1, 0):
            pltpu.make_async_remote_copy(
                src_ref=xsend, dst_ref=xslots.at[t, place], send_sem=xsend_sem, recv_sem=xrecv_sem.at[t],
                device_id=worker(prev_job, mate(d, job_core)), device_id_type=MESH).start()
        user_step()

        @pl.when(t == EPOCHS * blk_n - 1)
        def _():
            for q in (3, 1, 2):
                give_users(q).start()

            @pl.when(jnp.logical_not(has_own))
            def _():
                give_users(0).start()

        everyone = xslots.at[t]
        pltpu.make_async_copy(everyone, everyone, xsend_sem).wait()
        ahead.wait()
        pltpu.make_async_copy(everyone, everyone, xrecv_sem.at[t]).wait()
        return item_step(vslots[t], xslots[t])

    @pl.when(is_worker)
    def _():
        wt[...] = jnp.zeros_like(wt)
        await_pieces(ut, user_recv)

        @pl.when(jnp.logical_not(has_own))
        def _():
            pltpu.make_async_copy(vst, vst, item_recv).wait()

        for q in range(PIECES):
            halves(q)
        vst[...] = lax.fori_loop(0, EPOCHS * blk_n, sub_epoch, vst[...])
        for q in (3, 2, 1):
            give_items(q).start()

        @pl.when(jnp.logical_not(has_own))
        def _():
            give_items(0).start()

        @pl.when(ships)
        def _():
            ship(blk_n - 2).wait_send()
            ship(blk_n - 1).wait_send()

    @pl.when(ships)
    def _():
        send_users.wait_send()
        pltpu.make_async_copy(uret, uret, back_recv).wait()
        pltpu.make_async_copy(vret, vret, final_recv).wait()
        for g in range(GROUPS):
            ut_out[:, g * rows:(g + 1) * rows] = uret[g * rank:(g + 1) * rank, :]
        vt_out[0:half, :] = vret[:, 0:64]
        vt_out[half:rank, :] = vret[:, 64:128]

    @pl.when(gives_items)
    def _():
        send_items.wait_send()

    @pl.when(is_own)
    def _():
        for g in range(GROUPS):
            ut_out[:, g * rows:(g + 1) * rows] = ut[0, g * rank:(g + 1) * rank, :]
        vt_out[0:half, :] = vst[:, 0:64]
        vt_out[half:rank, :] = vst[:, 64:128]

    @pl.when(is_worker)
    def _():
        for q in (3, 2, 1):
            give_users(q).wait_send()
            give_items(q).wait_send()

        @pl.when(jnp.logical_not(has_own))
        def _():
            give_users(0).wait_send()
            give_items(0).wait_send()


def solution(mesh):
    blk_n = mesh.shape["blk"]
    sub_n = mesh.shape["sub"]
    row_spec = P(("rep", "blk", "sub"), None)
    item_spec = P(("rep", "blk"), None)

    def local_run(ratings, mask, user_init, item_init):
        users = ratings.shape[0]
        items, rank = item_init.shape
        big_side = max(items, sub_n * users)
        step_size = STEP_GAIN * math.sqrt(rank) / (math.sqrt(big_side) + math.sqrt(rank)) ** 2
        decay_coef = DECAY / step_size
        rows = users // GROUPS
        turns = EPOCHS * blk_n
        half = rank // 2
        wide_u, wide_i = GROUPS * rank, GROUPS * items
        vmem = pl.BlockSpec(memory_space=pltpu.VMEM)
        dma = pltpu.SemaphoreType.DMA
        ut, vt = pl.pallas_call(
            functools.partial(kernel, (blk_n, step_size, decay_coef)),
            out_shape=(jax.ShapeDtypeStruct((rank, users), jnp.float32), jax.ShapeDtypeStruct((rank, items), jnp.float32)),
            in_specs=[pl.BlockSpec(memory_space=pl.ANY)] * 4,
            out_specs=(vmem, vmem),
            scratch_shapes=[
                pltpu.VMEM((blk_n // 2, users, 128), jnp.float32),
                pltpu.VMEM((blk_n // 2, users, 128), jnp.int32),
                pltpu.VMEM((rank, users), jnp.float32),
                pltpu.VMEM((rank, items), jnp.float32),
                pltpu.VMEM((blk_n, rows, wide_i), jnp.float32),
                pltpu.VMEM((blk_n, PIECES, rows, wide_i), jnp.float32),
                pltpu.VMEM((wide_u, rows), jnp.float32),
                pltpu.VMEM((wide_u, rows), jnp.float32),
                pltpu.VMEM((half, 128), jnp.float32),
                pltpu.VMEM((half, 128), jnp.float32),
                pltpu.VMEM((PIECES, wide_u, rows), jnp.float32),
                pltpu.VMEM((PIECES * rows, wide_u), jnp.bfloat16),
                pltpu.VMEM((wide_u, PIECES * rows), jnp.bfloat16),
                pltpu.VMEM((wide_u, wide_i), jnp.bfloat16),
                pltpu.VMEM((PIECES * rows, wide_i), jnp.bfloat16),
                pltpu.VMEM((half, 128), jnp.float32),
                pltpu.VMEM((half, 128), jnp.float32),
                pltpu.VMEM((STEPS - 1, TEAM, half, 128), jnp.float32),
                pltpu.VMEM((turns, TEAM, half, 128), jnp.float32),
                pltpu.VMEM((turns, half, 128), jnp.float32),
                dma((3, blk_n // 2)),
                dma((blk_n,)), dma((blk_n,)),
                dma, dma, dma, dma,
                dma((PIECES,)), dma,
                dma((PIECES,)), dma,
                dma((STEPS - 1,)), dma((STEPS - 1,)),
                dma, dma((turns,)),
                dma, dma((turns,)),
                pltpu.SemaphoreType.REGULAR,
            ],
            compiler_params=pltpu.CompilerParams(collective_id=0, has_side_effects=True, vmem_limit_bytes=53 * 1024 * 1024),
        )(ratings, mask, pltpu.with_memory_space_constraint(user_init.T, pltpu.HBM), pltpu.with_memory_space_constraint(item_init.T, pltpu.HBM))
        return ut.T, vt.T

    return jax.shard_map(local_run, mesh=mesh, in_specs=(row_spec, row_spec, row_spec, item_spec), out_specs=(row_spec, item_spec), check_vma=False)
```

```python
import functools
import math

import jax
import jax.numpy as jnp
from jax import lax
from jax.experimental import pallas as pl
from jax.experimental.pallas import tpu as pltpu
from jax.sharding import PartitionSpec as P

STEPS = 4
EPOCHS = 2
STEP_GAIN = 0.4
DECAY = 0.002
GROUPS = 4
TEAM = 4
PIECES = 4
SPLIT = (3, 3, 2)
MESH = pl.DeviceIdType.MESH


def kernel(dims, r_hbm, m_hbm, u_hbm, v_hbm, ut_out, vt_out, rbuf, mbuf, ubuf, vbuf, packed, work, usrc, uret, vown, vret, ut, uh, uth, wt, err, vst,
           xsend, slots, xslots, vslots, load_sem, ship_send, ship_recv, user_send, user_recv, item_send, item_recv, back_send, back_recv,
           final_send, final_recv, send_sem, recv_sem, xsend_sem, xrecv_sem, vsend_sem, vrecv_sem, credit):
    blk_n, step_size, decay_coef = dims
    rank, users = ubuf.shape
    rows = users // GROUPS
    half = rank // 2
    pairs = blk_n // 2
    me_b = lax.axis_index("blk")
    me_s = lax.axis_index("sub")
    x, core = me_b // 2, me_b % 2
    z, y = me_s // 4, me_s % 4

    out_y = (y // 2 + core + x) % 2
    out_z = z // 2
    piece = 2 * out_y + out_z
    target = {"sub": (z + out_z * (3 - 2 * z)) * 4 + y + out_y * (3 - 2 * y), "blk": 2 * x + 1}
    is_own = jnp.logical_and(core == 1, piece == 0)
    ships = jnp.logical_not(is_own)
    is_worker = jnp.logical_and(core == 1, z < 2)
    job_core = (y // 2 + x) % 2
    job = 2 * x + job_core
    has_own = job_core == 1
    place = (z % 2) * 2 + y % 2

    def source(q):
        oy, oz = q // 2, q % 2
        return {"sub": (z + oz * (3 - 2 * z)) * 4 + y + oy * (3 - 2 * y), "blk": job}

    def worker(block, p):
        bx = block // 2
        return {"sub": (p // 2) * 4 + 2 * ((block % 2 + bx) % 2) + p % 2, "blk": 2 * bx + 1}

    prev_job = (job + blk_n - 1) % blk_n
    next_job = (job + 1) % blk_n

    def mate(d, flip=0):
        dz, dy = d // 2, d % 2
        pz, py = (place // 2 + dz) % 2, (place % 2 + dy + flip) % 2
        return pz * 2 + py

    def load(q, src, dst, kind):
        col = pl.multiple_of(((x + q) % pairs) * 128, 128)
        return pltpu.make_async_copy(src.at[:, pl.ds(col, 128)], dst.at[q], load_sem.at[kind, q])

    load_users = pltpu.make_async_copy(u_hbm, ubuf, load_sem.at[2, 0])
    load_items = pltpu.make_async_copy(v_hbm, vbuf, load_sem.at[2, 1])
    load_users.start()
    load_items.start()
    load(0, r_hbm, rbuf, 0).start()
    load(0, m_hbm, mbuf, 1).start()

    barrier = pltpu.get_barrier_semaphore()

    def greet(device):
        pl.semaphore_signal(barrier, inc=1, device_id=device, device_id_type=MESH)

    @pl.when(ships)
    def _():
        greet(target)

    @pl.when(is_worker)
    def _():
        for q in range(1, PIECES):
            greet(source(q))

        @pl.when(jnp.logical_not(has_own))
        def _():
            greet(source(0))

        for d in (3, 2, 1):
            greet(worker(job, mate(d)))
        for p in range(TEAM):
            greet(worker(prev_job, p))
            greet(worker(next_job, p))

    low = lax.broadcasted_iota(jnp.int32, (half, 128), 1) < 64
    left = lax.broadcasted_iota(jnp.int32, (rank, 128), 1) < 64

    load_users.wait()
    for g in range(GROUPS):
        usrc[g * rank:(g + 1) * rank, :] = ubuf[:, g * rows:(g + 1) * rows]
    load_items.wait()
    vown[:, 0:64] = vbuf[0:half, :]
    vown[:, 64:128] = vbuf[half:rank, :]

    @pl.when(jnp.logical_not(is_worker))
    def _():
        pl.semaphore_wait(barrier, 1)

    @pl.when(jnp.logical_and(is_worker, has_own))
    def _():
        pl.semaphore_wait(barrier, PIECES - 1 + TEAM - 1 + 2 * TEAM)

    @pl.when(jnp.logical_and(is_worker, jnp.logical_not(has_own)))
    def _():
        pl.semaphore_wait(barrier, PIECES + 1 + TEAM - 1 + 2 * TEAM)

    send_users = pltpu.make_async_remote_copy(
        src_ref=usrc, dst_ref=ut.at[piece], send_sem=user_send, recv_sem=user_recv, device_id=target, device_id_type=MESH)
    send_items = pltpu.make_async_remote_copy(
        src_ref=vown, dst_ref=vst, send_sem=item_send, recv_sem=item_recv, device_id=target, device_id_type=MESH)
    gives_items = jnp.logical_and(core == 0, piece == 0)

    @pl.when(ships)
    def _():
        send_users.start()

    @pl.when(gives_items)
    def _():
        send_items.start()

    def ship(k):
        column = (me_b + k) % blk_n
        return pltpu.make_async_remote_copy(
            src_ref=packed.at[column], dst_ref=work.at[column, piece], send_sem=ship_send.at[k], recv_sem=ship_recv.at[column],
            device_id=target, device_id_type=MESH)

    chunk = 64
    low_c = lax.broadcasted_iota(jnp.int32, (chunk, 128), 1) < 64

    def pack_pair(q):
        even = ((x + q) % pairs) * 2

        def pack_rows(c, carry):
            base = pl.multiple_of(c * chunk, chunk)
            for col in range(2):
                vals = []
                for g in (2 * col, 2 * col + 1):
                    src = pl.ds(g * rows + base, chunk)
                    vals.append(jnp.where(mbuf[q, src, :] != 0, rbuf[q, src, :], jnp.nan))
                x0, x1 = vals
                packed[even, pl.ds(base, chunk), col * 128:(col + 1) * 128] = jnp.where(low_c, x0, pltpu.roll(x1, 64, 1))
                packed[even + 1, pl.ds(base, chunk), col * 128:(col + 1) * 128] = jnp.where(low_c, pltpu.roll(x0, 64, 1), x1)
            return carry

        lax.fori_loop(0, rows // chunk, pack_rows, 0)

    load(0, r_hbm, rbuf, 0).wait()
    load(0, m_hbm, mbuf, 1).wait()
    for q in range(1, pairs):
        load(q, r_hbm, rbuf, 0).start()
        load(q, m_hbm, mbuf, 1).start()
    pack_pair(0)

    @pl.when(ships)
    def _():
        ship(0).start()

    def pack_rest(q, carry):
        load(q, r_hbm, rbuf, 0).wait()
        load(q, m_hbm, mbuf, 1).wait()
        pack_pair(q)
        return carry

    lax.fori_loop(1, pairs, pack_rest, 0)

    is_far = piece == 3

    @pl.when(is_far)
    def _():
        def ship_far(k, carry):
            pl.semaphore_wait(credit, 1)
            ship(k).start()
            ship(k - 1).wait_send()
            return carry

        lax.fori_loop(1, blk_n, ship_far, 0)
        ship(blk_n - 1).wait_send()

    @pl.when(jnp.logical_and(ships, jnp.logical_not(is_far)))
    def _():
        ship(1).start()

    @pl.when(jnp.logical_and(ships, jnp.logical_not(jnp.logical_or(is_worker, is_far))))
    def _():
        def ship_next(k, carry):
            ship(k - 2).wait_send()
            ship(k).start()
            return carry

        lax.fori_loop(2, blk_n, ship_next, 0)
        ship(blk_n - 2).wait_send()
        ship(blk_n - 1).wait_send()

    @pl.when(is_own)
    def _():
        def keep(column, carry):
            work[column, 0] = packed[column]
            return carry

        lax.fori_loop(0, blk_n, keep, 0)
        ut[0] = usrc[...]
        vst[...] = vown[...]

    def halves(q):
        new_half = ut[q].astype(jnp.bfloat16)
        uth[:, q * rows:(q + 1) * rows] = new_half
        uh[q * rows:(q + 1) * rows, :] = new_half.T

    def spread(vp):
        swapped = pltpu.roll(vp, 64, 1)
        full = jnp.concatenate([jnp.where(low, vp, swapped), jnp.where(low, swapped, vp)], axis=0)
        lo = jnp.where(left, full, 0.0).astype(jnp.bfloat16)
        hi = jnp.where(left, 0.0, full).astype(jnp.bfloat16)
        wt[0:rank, 0:128] = lo
        wt[rank:2 * rank, 0:128] = hi
        wt[2 * rank:3 * rank, 128:256] = lo
        wt[3 * rank:4 * rank, 128:256] = hi

    def partial(block):
        for q in range(PIECES):
            sl = slice(q * rows, (q + 1) * rows)
            predicted = jnp.dot(uh[sl, :], wt[...], preferred_element_type=jnp.float32)
            rate = work[block, q]
            err[sl, :] = jnp.where(rate == rate, predicted - rate, 0.0).astype(jnp.bfloat16)
        both = None
        start = 0
        for share in SPLIT:
            sl = slice(start, start + share * PIECES * rows // sum(SPLIT))
            start = sl.stop
            s = jnp.dot(uth[:, sl], err[sl, :], preferred_element_type=jnp.float32)
            s_lo = s[0:rank, 0:128] + s[2 * rank:3 * rank, 128:256]
            s_hi = s[rank:2 * rank, 0:128] + s[3 * rank:4 * rank, 128:256]
            part = jnp.where(left, s_lo, s_hi)
            both = part if both is None else both + part
        top, bottom = both[0:half], both[half:rank]
        return jnp.where(low, top, bottom) + pltpu.roll(jnp.where(low, bottom, top), 64, 1)

    def user_step():
        for q in range(PIECES):
            grad = lax.dot_general(wt[...], err[q * rows:(q + 1) * rows, :], (((1,), (1,)), ((), ())), preferred_element_type=jnp.float32)
            old = ut[q]
            ut[q] = old - step_size * (grad + decay_coef * old)
            halves(q)

    def item_step(old, parts):
        total = (parts[0] + parts[1]) + (parts[2] + parts[3])
        return old - step_size * (total + decay_coef * old)

    def await_pieces(buf, sem):
        @pl.when(has_own)
        def _():
            most = buf.at[pl.ds(1, PIECES - 1)]
            pltpu.make_async_copy(most, most, sem).wait()

        @pl.when(jnp.logical_not(has_own))
        def _():
            pltpu.make_async_copy(buf, buf, sem).wait()

    def give_users(q):
        return pltpu.make_async_remote_copy(
            src_ref=ut.at[q], dst_ref=uret, send_sem=back_send.at[q], recv_sem=back_recv, device_id=source(q), device_id_type=MESH)

    def give_items(q):
        return pltpu.make_async_remote_copy(
            src_ref=vst, dst_ref=vret, send_sem=final_send.at[q], recv_sem=final_recv, device_id=source(q), device_id_type=MESH)

    def sub_epoch(t, vp):
        block = (job + t) % blk_n

        @pl.when(t < blk_n)
        def _():
            await_pieces(work.at[block], ship_recv.at[block])

        for step in range(STEPS - 1):
            spread(vp)
            slots[step, place] = partial(block)
            for d in (3, 2, 1):
                pltpu.make_async_remote_copy(
                    src_ref=slots.at[step, place], dst_ref=slots.at[step, place], send_sem=send_sem.at[step], recv_sem=recv_sem.at[step],
                    device_id=worker(job, mate(d)), device_id_type=MESH).start()
            if step == 0:
                @pl.when(t < blk_n - 1)
                def _():
                    pl.semaphore_signal(credit, inc=1, device_id=source(3), device_id_type=MESH)

                @pl.when(jnp.logical_and(ships, t < blk_n - 2))
                def _():
                    ship(t).wait_send()
                    ship(t + 2).start()

            user_step()
            others = slots.at[step, pl.ds(0, TEAM - 1)]
            pltpu.make_async_copy(others, others, send_sem.at[step]).wait()
            pltpu.make_async_copy(others, others, recv_sem.at[step]).wait()
            vp = item_step(vp, slots[step])
        vst[...] = vp
        ahead = pltpu.make_async_remote_copy(
            src_ref=vst, dst_ref=vslots.at[t], send_sem=vsend_sem, recv_sem=vrecv_sem.at[t],
            device_id=worker(prev_job, place), device_id_type=MESH)
        ahead.start()
        spread(vp)
        xsend[...] = partial(block)
        for d in (3, 2, 1, 0):
            pltpu.make_async_remote_copy(
                src_ref=xsend, dst_ref=xslots.at[t, place], send_sem=xsend_sem, recv_sem=xrecv_sem.at[t],
                device_id=worker(prev_job, mate(d, job_core)), device_id_type=MESH).start()
        user_step()

        @pl.when(t == EPOCHS * blk_n - 1)
        def _():
            for q in (3, 1, 2):
                give_users(q).start()

            @pl.when(jnp.logical_not(has_own))
            def _():
                give_users(0).start()

        everyone = xslots.at[t]
        pltpu.make_async_copy(everyone, everyone, xsend_sem).wait()
        ahead.wait()
        pltpu.make_async_copy(everyone, everyone, xrecv_sem.at[t]).wait()
        return item_step(vslots[t], xslots[t])

    @pl.when(is_worker)
    def _():
        wt[...] = jnp.zeros_like(wt)
        await_pieces(ut, user_recv)

        @pl.when(jnp.logical_not(has_own))
        def _():
            pltpu.make_async_copy(vst, vst, item_recv).wait()

        for q in range(PIECES):
            halves(q)
        vst[...] = lax.fori_loop(0, EPOCHS * blk_n, sub_epoch, vst[...])
        for q in (3, 2, 1):
            give_items(q).start()

        @pl.when(jnp.logical_not(has_own))
        def _():
            give_items(0).start()

        @pl.when(ships)
        def _():
            ship(blk_n - 2).wait_send()
            ship(blk_n - 1).wait_send()

    @pl.when(ships)
    def _():
        send_users.wait_send()
        pltpu.make_async_copy(uret, uret, back_recv).wait()
        pltpu.make_async_copy(vret, vret, final_recv).wait()
        for g in range(GROUPS):
            ut_out[:, g * rows:(g + 1) * rows] = uret[g * rank:(g + 1) * rank, :]
        vt_out[0:half, :] = vret[:, 0:64]
        vt_out[half:rank, :] = vret[:, 64:128]

    @pl.when(gives_items)
    def _():
        send_items.wait_send()

    @pl.when(is_own)
    def _():
        for g in range(GROUPS):
            ut_out[:, g * rows:(g + 1) * rows] = ut[0, g * rank:(g + 1) * rank, :]
        vt_out[0:half, :] = vst[:, 0:64]
        vt_out[half:rank, :] = vst[:, 64:128]

    @pl.when(is_worker)
    def _():
        for q in (3, 2, 1):
            give_users(q).wait_send()
            give_items(q).wait_send()

        @pl.when(jnp.logical_not(has_own))
        def _():
            give_users(0).wait_send()
            give_items(0).wait_send()


def solution(mesh):
    blk_n = mesh.shape["blk"]
    sub_n = mesh.shape["sub"]
    row_spec = P(("rep", "blk", "sub"), None)
    item_spec = P(("rep", "blk"), None)

    def local_run(ratings, mask, user_init, item_init):
        users = ratings.shape[0]
        items, rank = item_init.shape
        big_side = max(items, sub_n * users)
        step_size = STEP_GAIN * math.sqrt(rank) / (math.sqrt(big_side) + math.sqrt(rank)) ** 2
        decay_coef = DECAY / step_size
        rows = users // GROUPS
        turns = EPOCHS * blk_n
        half = rank // 2
        wide_u, wide_i = GROUPS * rank, GROUPS * items
        vmem = pl.BlockSpec(memory_space=pltpu.VMEM)
        dma = pltpu.SemaphoreType.DMA
        ut, vt = pl.pallas_call(
            functools.partial(kernel, (blk_n, step_size, decay_coef)),
            out_shape=(jax.ShapeDtypeStruct((rank, users), jnp.float32), jax.ShapeDtypeStruct((rank, items), jnp.float32)),
            in_specs=[pl.BlockSpec(memory_space=pl.ANY)] * 4,
            out_specs=(vmem, vmem),
            scratch_shapes=[
                pltpu.VMEM((blk_n // 2, users, 128), jnp.float32),
                pltpu.VMEM((blk_n // 2, users, 128), jnp.int32),
                pltpu.VMEM((rank, users), jnp.float32),
                pltpu.VMEM((rank, items), jnp.float32),
                pltpu.VMEM((blk_n, rows, wide_i), jnp.float32),
                pltpu.VMEM((blk_n, PIECES, rows, wide_i), jnp.float32),
                pltpu.VMEM((wide_u, rows), jnp.float32),
                pltpu.VMEM((wide_u, rows), jnp.float32),
                pltpu.VMEM((half, 128), jnp.float32),
                pltpu.VMEM((half, 128), jnp.float32),
                pltpu.VMEM((PIECES, wide_u, rows), jnp.float32),
                pltpu.VMEM((PIECES * rows, wide_u), jnp.bfloat16),
                pltpu.VMEM((wide_u, PIECES * rows), jnp.bfloat16),
                pltpu.VMEM((wide_u, wide_i), jnp.bfloat16),
                pltpu.VMEM((PIECES * rows, wide_i), jnp.bfloat16),
                pltpu.VMEM((half, 128), jnp.float32),
                pltpu.VMEM((half, 128), jnp.float32),
                pltpu.VMEM((STEPS - 1, TEAM, half, 128), jnp.float32),
                pltpu.VMEM((turns, TEAM, half, 128), jnp.float32),
                pltpu.VMEM((turns, half, 128), jnp.float32),
                dma((3, blk_n // 2)),
                dma((blk_n,)), dma((blk_n,)),
                dma, dma, dma, dma,
                dma((PIECES,)), dma,
                dma((PIECES,)), dma,
                dma((STEPS - 1,)), dma((STEPS - 1,)),
                dma, dma((turns,)),
                dma, dma((turns,)),
                pltpu.SemaphoreType.REGULAR,
            ],
            compiler_params=pltpu.CompilerParams(collective_id=0, has_side_effects=True, vmem_limit_bytes=53 * 1024 * 1024),
        )(ratings, mask, pltpu.with_memory_space_constraint(user_init.T, pltpu.HBM), pltpu.with_memory_space_constraint(item_init.T, pltpu.HBM))
        return ut.T, vt.T

    return jax.shard_map(local_run, mesh=mesh, in_specs=(row_spec, row_spec, row_spec, item_spec), out_specs=(row_spec, item_spec), check_vma=False)
```

```python
import functools
import math

import jax
import jax.numpy as jnp
from jax import lax
from jax.experimental import pallas as pl
from jax.experimental.pallas import tpu as pltpu
from jax.sharding import PartitionSpec as P

STEPS = 4
EPOCHS = 2
STEP_GAIN = 0.4
DECAY = 0.002
GROUPS = 4
TEAM = 4
PIECES = 4
SPLIT = (3, 3, 2)
MESH = pl.DeviceIdType.MESH


def kernel(dims, r_hbm, m_hbm, u_hbm, v_hbm, ut_out, vt_out, rbuf, mbuf, ubuf, vbuf, packed, work, usrc, uret, vown, vret, ut, uh, uth, wt, err, vst,
           xsend, slots, xslots, vslots, load_sem, ship_send, ship_recv, user_send, user_recv, item_send, item_recv, back_send, back_recv,
           final_send, final_recv, send_sem, recv_sem, xsend_sem, xrecv_sem, vsend_sem, vrecv_sem, credit):
    blk_n, step_size, decay_coef = dims
    rank, users = ubuf.shape
    rows = users // GROUPS
    half = rank // 2
    pairs = blk_n // 2
    me_b = lax.axis_index("blk")
    me_s = lax.axis_index("sub")
    x, core = me_b // 2, me_b % 2
    z, y = me_s // 4, me_s % 4

    out_y = (y // 2 + core + x) % 2
    out_z = z // 2
    piece = 2 * out_y + out_z
    target = {"sub": (z + out_z * (3 - 2 * z)) * 4 + y + out_y * (3 - 2 * y), "blk": 2 * x + 1}
    is_own = jnp.logical_and(core == 1, piece == 0)
    ships = jnp.logical_not(is_own)
    is_worker = jnp.logical_and(core == 1, z < 2)
    job_core = (y // 2 + x) % 2
    job = 2 * x + job_core
    has_own = job_core == 1
    place = (z % 2) * 2 + y % 2

    def source(q):
        oy, oz = q // 2, q % 2
        return {"sub": (z + oz * (3 - 2 * z)) * 4 + y + oy * (3 - 2 * y), "blk": job}

    def worker(block, p):
        bx = block // 2
        return {"sub": (p // 2) * 4 + 2 * ((block % 2 + bx) % 2) + p % 2, "blk": 2 * bx + 1}

    prev_job = (job + blk_n - 1) % blk_n
    next_job = (job + 1) % blk_n

    def mate(d, flip=0):
        dz, dy = d // 2, d % 2
        pz, py = (place // 2 + dz) % 2, (place % 2 + dy + flip) % 2
        return pz * 2 + py

    def load(q, src, dst, kind):
        col = pl.multiple_of(((x + q) % pairs) * 128, 128)
        return pltpu.make_async_copy(src.at[:, pl.ds(col, 128)], dst.at[q], load_sem.at[kind, q])

    load_users = pltpu.make_async_copy(u_hbm, ubuf, load_sem.at[2, 0])
    load_items = pltpu.make_async_copy(v_hbm, vbuf, load_sem.at[2, 1])
    load_users.start()
    load_items.start()
    load(0, r_hbm, rbuf, 0).start()
    load(0, m_hbm, mbuf, 1).start()

    barrier = pltpu.get_barrier_semaphore()

    def greet(device):
        pl.semaphore_signal(barrier, inc=1, device_id=device, device_id_type=MESH)

    @pl.when(ships)
    def _():
        greet(target)

    @pl.when(is_worker)
    def _():
        for q in range(1, PIECES):
            greet(source(q))

        @pl.when(jnp.logical_not(has_own))
        def _():
            greet(source(0))

        for d in (3, 2, 1):
            greet(worker(job, mate(d)))
        for p in range(TEAM):
            greet(worker(prev_job, p))
            greet(worker(next_job, p))

    low = lax.broadcasted_iota(jnp.int32, (half, 128), 1) < 64
    left = lax.broadcasted_iota(jnp.int32, (rank, 128), 1) < 64

    load_users.wait()
    for g in range(GROUPS):
        usrc[g * rank:(g + 1) * rank, :] = ubuf[:, g * rows:(g + 1) * rows]
    load_items.wait()
    vown[:, 0:64] = vbuf[0:half, :]
    vown[:, 64:128] = vbuf[half:rank, :]

    @pl.when(jnp.logical_not(is_worker))
    def _():
        pl.semaphore_wait(barrier, 1)

    @pl.when(jnp.logical_and(is_worker, has_own))
    def _():
        pl.semaphore_wait(barrier, PIECES - 1 + TEAM - 1 + 2 * TEAM)

    @pl.when(jnp.logical_and(is_worker, jnp.logical_not(has_own)))
    def _():
        pl.semaphore_wait(barrier, PIECES + 1 + TEAM - 1 + 2 * TEAM)

    send_users = pltpu.make_async_remote_copy(
        src_ref=usrc, dst_ref=ut.at[piece], send_sem=user_send, recv_sem=user_recv, device_id=target, device_id_type=MESH)
    send_items = pltpu.make_async_remote_copy(
        src_ref=vown, dst_ref=vst, send_sem=item_send, recv_sem=item_recv, device_id=target, device_id_type=MESH)
    gives_items = jnp.logical_and(core == 0, piece == 0)

    @pl.when(ships)
    def _():
        send_users.start()

    @pl.when(gives_items)
    def _():
        send_items.start()

    def ship(k):
        column = (me_b + k) % blk_n
        return pltpu.make_async_remote_copy(
            src_ref=packed.at[column], dst_ref=work.at[column, piece], send_sem=ship_send.at[k], recv_sem=ship_recv.at[column],
            device_id=target, device_id_type=MESH)

    chunk = 64
    low_c = lax.broadcasted_iota(jnp.int32, (chunk, 128), 1) < 64

    def pack_pair(q):
        even = ((x + q) % pairs) * 2

        def pack_rows(c, carry):
            base = pl.multiple_of(c * chunk, chunk)
            for col in range(2):
                vals = []
                for g in (2 * col, 2 * col + 1):
                    src = pl.ds(g * rows + base, chunk)
                    vals.append(jnp.where(mbuf[q, src, :] != 0, rbuf[q, src, :], jnp.nan))
                x0, x1 = vals
                packed[even, pl.ds(base, chunk), col * 128:(col + 1) * 128] = jnp.where(low_c, x0, pltpu.roll(x1, 64, 1))
                packed[even + 1, pl.ds(base, chunk), col * 128:(col + 1) * 128] = jnp.where(low_c, pltpu.roll(x0, 64, 1), x1)
            return carry

        lax.fori_loop(0, rows // chunk, pack_rows, 0)

    load(0, r_hbm, rbuf, 0).wait()
    load(0, m_hbm, mbuf, 1).wait()
    for q in range(1, pairs):
        load(q, r_hbm, rbuf, 0).start()
        load(q, m_hbm, mbuf, 1).start()
    pack_pair(0)

    @pl.when(ships)
    def _():
        ship(0).start()

    def pack_rest(q, carry):
        load(q, r_hbm, rbuf, 0).wait()
        load(q, m_hbm, mbuf, 1).wait()
        pack_pair(q)
        return carry

    lax.fori_loop(1, pairs, pack_rest, 0)

    is_far = piece == 3

    @pl.when(is_far)
    def _():
        def ship_far(k, carry):
            pl.semaphore_wait(credit, 1)
            ship(k).start()
            ship(k - 1).wait_send()
            return carry

        lax.fori_loop(1, blk_n, ship_far, 0)
        ship(blk_n - 1).wait_send()

    @pl.when(jnp.logical_and(ships, jnp.logical_not(is_far)))
    def _():
        ship(1).start()

    @pl.when(jnp.logical_and(ships, jnp.logical_not(jnp.logical_or(is_worker, is_far))))
    def _():
        def ship_next(k, carry):
            ship(k - 2).wait_send()
            ship(k).start()
            return carry

        lax.fori_loop(2, blk_n, ship_next, 0)
        ship(blk_n - 2).wait_send()
        ship(blk_n - 1).wait_send()

    @pl.when(is_own)
    def _():
        def keep(column, carry):
            work[column, 0] = packed[column]
            return carry

        lax.fori_loop(0, blk_n, keep, 0)
        ut[0] = usrc[...]
        vst[...] = vown[...]

    def halves(q):
        new_half = ut[q].astype(jnp.bfloat16)
        uth[:, q * rows:(q + 1) * rows] = new_half
        uh[q * rows:(q + 1) * rows, :] = new_half.T

    def spread(vp):
        swapped = pltpu.roll(vp, 64, 1)
        full = jnp.concatenate([jnp.where(low, vp, swapped), jnp.where(low, swapped, vp)], axis=0)
        lo = jnp.where(left, full, 0.0).astype(jnp.bfloat16)
        hi = jnp.where(left, 0.0, full).astype(jnp.bfloat16)
        wt[0:rank, 0:128] = lo
        wt[rank:2 * rank, 0:128] = hi
        wt[2 * rank:3 * rank, 128:256] = lo
        wt[3 * rank:4 * rank, 128:256] = hi

    def partial(block):
        for q in range(PIECES):
            sl = slice(q * rows, (q + 1) * rows)
            predicted = jnp.dot(uh[sl, :], wt[...], preferred_element_type=jnp.float32)
            rate = work[block, q]
            err[sl, :] = jnp.where(rate == rate, predicted - rate, 0.0).astype(jnp.bfloat16)
        both = None
        start = 0
        for share in SPLIT:
            sl = slice(start, start + share * PIECES * rows // sum(SPLIT))
            start = sl.stop
            s = jnp.dot(uth[:, sl], err[sl, :], preferred_element_type=jnp.float32)
            s_lo = s[0:rank, 0:128] + s[2 * rank:3 * rank, 128:256]
            s_hi = s[rank:2 * rank, 0:128] + s[3 * rank:4 * rank, 128:256]
            part = jnp.where(left, s_lo, s_hi)
            both = part if both is None else both + part
        top, bottom = both[0:half], both[half:rank]
        return jnp.where(low, top, bottom) + pltpu.roll(jnp.where(low, bottom, top), 64, 1)

    def user_step():
        for q in range(PIECES):
            grad = lax.dot_general(wt[...], err[q * rows:(q + 1) * rows, :], (((1,), (1,)), ((), ())), preferred_element_type=jnp.float32)
            old = ut[q]
            ut[q] = old - step_size * (grad + decay_coef * old)
            halves(q)

    def item_step(old, parts):
        total = (parts[0] + parts[1]) + (parts[2] + parts[3])
        return old - step_size * (total + decay_coef * old)

    def await_pieces(buf, sem):
        @pl.when(has_own)
        def _():
            most = buf.at[pl.ds(1, PIECES - 1)]
            pltpu.make_async_copy(most, most, sem).wait()

        @pl.when(jnp.logical_not(has_own))
        def _():
            pltpu.make_async_copy(buf, buf, sem).wait()

    def give_users(q):
        return pltpu.make_async_remote_copy(
            src_ref=ut.at[q], dst_ref=uret, send_sem=back_send.at[q], recv_sem=back_recv, device_id=source(q), device_id_type=MESH)

    def give_items(q):
        return pltpu.make_async_remote_copy(
            src_ref=vst, dst_ref=vret, send_sem=final_send.at[q], recv_sem=final_recv, device_id=source(q), device_id_type=MESH)

    def sub_epoch(t, vp):
        block = (job + t) % blk_n

        @pl.when(t < blk_n)
        def _():
            await_pieces(work.at[block], ship_recv.at[block])

        for step in range(STEPS - 1):
            spread(vp)
            slots[step, place] = partial(block)
            for d in (3, 2, 1):
                pltpu.make_async_remote_copy(
                    src_ref=slots.at[step, place], dst_ref=slots.at[step, place], send_sem=send_sem.at[step], recv_sem=recv_sem.at[step],
                    device_id=worker(job, mate(d)), device_id_type=MESH).start()
            if step == 0:
                @pl.when(t < blk_n - 1)
                def _():
                    pl.semaphore_signal(credit, inc=1, device_id=source(3), device_id_type=MESH)

                @pl.when(jnp.logical_and(ships, t < blk_n - 2))
                def _():
                    ship(t).wait_send()
                    ship(t + 2).start()

            user_step()
            others = slots.at[step, pl.ds(0, TEAM - 1)]
            pltpu.make_async_copy(others, others, send_sem.at[step]).wait()
            pltpu.make_async_copy(others, others, recv_sem.at[step]).wait()
            vp = item_step(vp, slots[step])
        spread(vp)
        vst[...] = vp
        ahead = pltpu.make_async_remote_copy(
            src_ref=vst, dst_ref=vslots.at[t], send_sem=vsend_sem, recv_sem=vrecv_sem.at[t],
            device_id=worker(prev_job, place), device_id_type=MESH)
        ahead.start()
        xsend[...] = partial(block)
        for d in (3, 2, 1, 0):
            pltpu.make_async_remote_copy(
                src_ref=xsend, dst_ref=xslots.at[t, place], send_sem=xsend_sem, recv_sem=xrecv_sem.at[t],
                device_id=worker(prev_job, mate(d, job_core)), device_id_type=MESH).start()
        user_step()

        @pl.when(t == EPOCHS * blk_n - 1)
        def _():
            for q in (3, 1, 2):
                give_users(q).start()

            @pl.when(jnp.logical_not(has_own))
            def _():
                give_users(0).start()

        everyone = xslots.at[t]
        pltpu.make_async_copy(everyone, everyone, xsend_sem).wait()
        ahead.wait()
        pltpu.make_async_copy(everyone, everyone, xrecv_sem.at[t]).wait()
        return item_step(vslots[t], xslots[t])

    @pl.when(is_worker)
    def _():
        wt[...] = jnp.zeros_like(wt)
        await_pieces(ut, user_recv)

        @pl.when(jnp.logical_not(has_own))
        def _():
            pltpu.make_async_copy(vst, vst, item_recv).wait()

        for q in range(PIECES):
            halves(q)
        vst[...] = lax.fori_loop(0, EPOCHS * blk_n, sub_epoch, vst[...])
        for q in (3, 2, 1):
            give_items(q).start()

        @pl.when(jnp.logical_not(has_own))
        def _():
            give_items(0).start()

        @pl.when(ships)
        def _():
            ship(blk_n - 2).wait_send()
            ship(blk_n - 1).wait_send()

    @pl.when(ships)
    def _():
        send_users.wait_send()
        pltpu.make_async_copy(uret, uret, back_recv).wait()
        pltpu.make_async_copy(vret, vret, final_recv).wait()
        for g in range(GROUPS):
            ut_out[:, g * rows:(g + 1) * rows] = uret[g * rank:(g + 1) * rank, :]
        vt_out[0:half, :] = vret[:, 0:64]
        vt_out[half:rank, :] = vret[:, 64:128]

    @pl.when(gives_items)
    def _():
        send_items.wait_send()

    @pl.when(is_own)
    def _():
        for g in range(GROUPS):
            ut_out[:, g * rows:(g + 1) * rows] = ut[0, g * rank:(g + 1) * rank, :]
        vt_out[0:half, :] = vst[:, 0:64]
        vt_out[half:rank, :] = vst[:, 64:128]

    @pl.when(is_worker)
    def _():
        for q in (3, 2, 1):
            give_users(q).wait_send()
            give_items(q).wait_send()

        @pl.when(jnp.logical_not(has_own))
        def _():
            give_users(0).wait_send()
            give_items(0).wait_send()


def solution(mesh):
    blk_n = mesh.shape["blk"]
    sub_n = mesh.shape["sub"]
    row_spec = P(("rep", "blk", "sub"), None)
    item_spec = P(("rep", "blk"), None)

    def local_run(ratings, mask, user_init, item_init):
        users = ratings.shape[0]
        items, rank = item_init.shape
        big_side = max(items, sub_n * users)
        step_size = STEP_GAIN * math.sqrt(rank) / (math.sqrt(big_side) + math.sqrt(rank)) ** 2
        decay_coef = DECAY / step_size
        rows = users // GROUPS
        turns = EPOCHS * blk_n
        half = rank // 2
        wide_u, wide_i = GROUPS * rank, GROUPS * items
        vmem = pl.BlockSpec(memory_space=pltpu.VMEM)
        dma = pltpu.SemaphoreType.DMA
        ut, vt = pl.pallas_call(
            functools.partial(kernel, (blk_n, step_size, decay_coef)),
            out_shape=(jax.ShapeDtypeStruct((rank, users), jnp.float32), jax.ShapeDtypeStruct((rank, items), jnp.float32)),
            in_specs=[pl.BlockSpec(memory_space=pl.ANY)] * 4,
            out_specs=(vmem, vmem),
            scratch_shapes=[
                pltpu.VMEM((blk_n // 2, users, 128), jnp.float32),
                pltpu.VMEM((blk_n // 2, users, 128), jnp.int32),
                pltpu.VMEM((rank, users), jnp.float32),
                pltpu.VMEM((rank, items), jnp.float32),
                pltpu.VMEM((blk_n, rows, wide_i), jnp.float32),
                pltpu.VMEM((blk_n, PIECES, rows, wide_i), jnp.float32),
                pltpu.VMEM((wide_u, rows), jnp.float32),
                pltpu.VMEM((wide_u, rows), jnp.float32),
                pltpu.VMEM((half, 128), jnp.float32),
                pltpu.VMEM((half, 128), jnp.float32),
                pltpu.VMEM((PIECES, wide_u, rows), jnp.float32),
                pltpu.VMEM((PIECES * rows, wide_u), jnp.bfloat16),
                pltpu.VMEM((wide_u, PIECES * rows), jnp.bfloat16),
                pltpu.VMEM((wide_u, wide_i), jnp.bfloat16),
                pltpu.VMEM((PIECES * rows, wide_i), jnp.bfloat16),
                pltpu.VMEM((half, 128), jnp.float32),
                pltpu.VMEM((half, 128), jnp.float32),
                pltpu.VMEM((STEPS - 1, TEAM, half, 128), jnp.float32),
                pltpu.VMEM((turns, TEAM, half, 128), jnp.float32),
                pltpu.VMEM((turns, half, 128), jnp.float32),
                dma((3, blk_n // 2)),
                dma((blk_n,)), dma((blk_n,)),
                dma, dma, dma, dma,
                dma((PIECES,)), dma,
                dma((PIECES,)), dma,
                dma((STEPS - 1,)), dma((STEPS - 1,)),
                dma, dma((turns,)),
                dma, dma((turns,)),
                pltpu.SemaphoreType.REGULAR,
            ],
            compiler_params=pltpu.CompilerParams(collective_id=0, has_side_effects=True, vmem_limit_bytes=53 * 1024 * 1024),
        )(ratings, mask, pltpu.with_memory_space_constraint(user_init.T, pltpu.HBM), pltpu.with_memory_space_constraint(item_init.T, pltpu.HBM))
        return ut.T, vt.T

    return jax.shard_map(local_run, mesh=mesh, in_specs=(row_spec, row_spec, row_spec, item_spec), out_specs=(row_spec, item_spec), check_vma=False)
```
